512 devices in a mesh: grp: 16 (over z), row: 32 (over x, y, core).
Axes of the slice: x: 4, y: 4, z: 16, core: 2. Of those that a mesh axis runs over, the one named last changes fastest.
Arguments:
- a_pieces: bfloat16 [16, 2048, 4096], P('grp', 'row'), as said below
- touched: int32 [16, 2048], P('grp', 'row'), may hold values from 0 to 7
- slot_row: int32 [2048], P('row'), may hold values from 0 to 2047, as said below
- x_blocks: bfloat16 [128, 64, 64], P('grp'), as said below
- z_inverse: bfloat16 [128, 64, 64], P('grp'), as said below
- block_class: int32 [128], P('grp'), may hold values from 0 to 1
Outputs:
- schur: float32 [2048, 2048], P('row', 'grp')
The draws below stay inside these ranges and needn't reach their ends.
Inputs may be any that keep to these rules, and one draw needn't show every extreme that they name: `slot_row`: A permutation of the constraints. The 64 slots of one index r of row (slots r * 64 onward) hold, of the constraints o * 64 to (o + 1) * 64 - 1 of each index o, either none or exactly 4. `a_pieces`: each piece read as a 64 x 64 matrix is symmetric. `x_blocks`: each block is symmetric positive definite. `z_inverse`: each block is symmetric positive definite.
All inputs are finite; a program needn't handle non-finite values.
Results may differ from the reference program's by a relative error of at most 0.0008.
Values may be sent and summed in bfloat16 or wider, within the bound.
No kernel may reach another device: no remote copies, remote signals or barrier semaphores. Data moves between devices by JAX's collectives and lax.ppermute only.
A program may use at most 64 MiB of HBM per device.

```python
import math
import jax
import jax.numpy as jnp
import numpy as np
from jax import lax

NB = 64
BLK_DEV = 8
ROWS_DEV = 64
CAP = 4
M = 2048
BLOCKS = 128
N_GRP = 16


def definite_blocks(key):
    raw = jax.random.normal(key, (BLOCKS, NB, NB), jnp.float32) / math.sqrt(NB)
    gram = jnp.einsum('kab,kcb->kac', raw, raw, precision=lax.Precision.HIGHEST)
    gram = 0.5 * (gram + jnp.swapaxes(gram, 1, 2)) + 0.5 * jnp.eye(NB, dtype=jnp.float32)[None]
    return gram.astype(jnp.bfloat16)


def draw_x_blocks(key, part):
    return definite_blocks(jax.random.fold_in(key, 11))


def draw_z_inverse(key, part):
    return definite_blocks(jax.random.fold_in(key, 23))


def draw_a_pieces(key, part):
    groups = BLOCKS // BLK_DEV
    raw = jax.random.normal(jax.random.fold_in(key, 31), (groups, M, NB, NB), jnp.float32)
    symmetric = (raw + jnp.swapaxes(raw, 2, 3)) / math.sqrt(2.0) / math.sqrt(8.0 * NB)
    return symmetric.reshape(groups, M, NB * NB).astype(jnp.bfloat16)


def shuffled(subkey):
    return jax.random.permutation(subkey, ROWS_DEV)


def place_value(order, value, position):
    where_now = jnp.argmax((order == value).astype(jnp.int32)).astype(jnp.int32)
    displaced = order[position]
    order = order.at[where_now].set(displaced)
    return order.at[position].set(value)


def draw_slot_row(key, part):
    devices = M // ROWS_DEV
    key_one, key_two = jax.random.split(jax.random.fold_in(key, 41))
    mixed = jax.random.permutation(key_one, devices)
    rotated = (mixed - mixed[0] + devices // 2) % devices
    rotated = place_value(rotated, 1, 1)
    rotated = place_value(rotated, devices - 1, 2)
    shifts = rotated[:ROWS_DEV // CAP]
    offsets = jnp.repeat(shifts, CAP)
    orders = jax.vmap(shuffled)(jax.random.split(key_two, devices))
    sources = jnp.arange(devices, dtype=jnp.int32)[:, None]
    owners = (sources - offsets[orders]) % devices
    return (owners * ROWS_DEV + orders).reshape(-1).astype(jnp.int32)


def with_ends(drawn, rng, smallest, high):
    longest = drawn.shape.index(max(drawn.shape))
    spots = []
    for shift in (0, 1):
        where = [jax.random.randint(jax.random.fold_in(rng, axis), (), 0, length) for axis, length in enumerate(drawn.shape)]
        where[longest] = (where[longest] + shift) % drawn.shape[longest]
        spots.append(tuple(where))
    return drawn.at[spots[0]].set(smallest).at[spots[1]].set(high)


def cumulative_ranks(amount, skew):
    weights = [(1 << 20) // math.isqrt(standing ** skew) + 1 for standing in range(1, amount + 1)]
    scale = 1 + sum(weights) // (1 << 30)
    return np.cumsum(np.array([max(1, weight // scale) for weight in weights]))


def ranked_ids(key, dims, count, slope):
    grid = cumulative_ranks(count, slope)
    lot = jax.random.randint(jax.random.fold_in(key, 1), dims, 0, int(grid[count - 1]))
    rank = jnp.searchsorted(jnp.asarray(grid, jnp.int32), lot, side="right")
    return jax.random.permutation(jax.random.fold_in(key, 2), count)[rank].astype(jnp.int32)


def setup_inputs(seed: int = 0) -> dict:
    splits = jax.random.split(jax.random.key(seed), 7)
    a_pieces = draw_a_pieces(jax.random.fold_in(splits[6], 71), 0)
    touched = with_ends(ranked_ids(splits[1], (N_GRP, M), BLK_DEV, 2), jax.random.fold_in(splits[1], 3), 0, BLK_DEV - 1).astype(jnp.int32)
    slot_row = draw_slot_row(jax.random.fold_in(splits[6], 71), 0)
    x_blocks = draw_x_blocks(jax.random.fold_in(splits[6], 71), 0)
    z_inverse = draw_z_inverse(jax.random.fold_in(splits[6], 71), 0)
    block_class = with_ends(jax.random.randint(splits[5], (BLOCKS,), 0, 2), jax.random.fold_in(splits[5], 1), 0, 1).astype(jnp.int32)
    return {"a_pieces": a_pieces, "touched": touched, "slot_row": slot_row, "x_blocks": x_blocks, "z_inverse": z_inverse, "block_class": block_class}


def masked_blocks(blocks, block_class):
    positions = jnp.arange(NB)
    active = (NB // 2) * (1 + block_class)
    inside = (positions[None, :, None] < active[:, None, None]) & (positions[None, None, :] < active[:, None, None])
    return jnp.where(inside, blocks, jnp.zeros_like(blocks))


def reference(a_pieces, touched, slot_row, x_blocks, z_inverse, block_class):
    x_masked = masked_blocks(x_blocks, block_class).reshape(N_GRP, BLK_DEV, NB, NB)
    z_masked = masked_blocks(z_inverse, block_class).reshape(N_GRP, BLK_DEV, NB, NB)

    def group_step(running, group_args):
        a_group, group_kinds, x_group, z_group = group_args
        pieces = a_group.reshape(M, NB, NB).astype(jnp.float32)
        left_part = jnp.einsum("rab,rbc->rac", x_group[group_kinds].astype(jnp.float32), pieces,
                               precision=lax.Precision.HIGHEST).astype(jnp.bfloat16)
        product = jnp.einsum("rab,rbc->rac", left_part.astype(jnp.float32), z_group[group_kinds].astype(jnp.float32),
                             precision=lax.Precision.HIGHEST).astype(jnp.bfloat16)
        scores = jnp.dot(product.reshape(M, NB * NB).astype(jnp.float32), a_group.astype(jnp.float32).T,
                         precision=lax.Precision.HIGHEST)
        scores = jnp.where(group_kinds[:, None] == group_kinds[None, :], scores, jnp.zeros_like(scores))
        return running + scores, None

    start_sum = jnp.zeros((M, M), jnp.float32)
    schur_slots, unused = lax.scan(group_step, start_sum, (a_pieces, touched, x_masked, z_masked))
    inverse = jnp.zeros((M,), jnp.int32).at[slot_row].set(jnp.arange(M, dtype=jnp.int32))
    return schur_slots[inverse][:, inverse]
```

```python
import functools
import jax
import jax.numpy as jnp
from jax import lax
from jax.experimental import pallas as pl
from jax.experimental.pallas import tpu as pltpu
from jax.sharding import PartitionSpec as P

F32 = jnp.float32
BF16 = jnp.bfloat16
HI = lax.Precision.HIGHEST
NB = 64
CHUNKS = 17
WIDTH = CHUNKS * 128
ROWS = 64
SIDE = 4
DEPTH = 80
Z_TYPE = jnp.float32
VMEM = pl.BlockSpec(memory_space=pltpu.VMEM)
SMEM = pl.BlockSpec(memory_space=pltpu.SMEM)


def iota(shape, dim):
    return lax.broadcasted_iota(jnp.int32, shape, dim)


def ones_where(cond, dtype=F32):
    return jnp.where(cond, 1.0, 0.0).astype(dtype)


def nt(a, b, precision=None):
    return lax.dot_general(a, b, (((1,), (1,)), ((), ())), precision=precision, preferred_element_type=F32)


def tn(a, b, precision=None):
    return lax.dot_general(a, b, (((0,), (0,)), ((), ())), precision=precision, preferred_element_type=F32)


def nn(a, b, precision=None):
    return lax.dot_general(a, b, (((1,), (0,)), ((), ())), precision=precision, preferred_element_type=F32)


def folded(read, weigh):
    lane = iota((ROWS, 128), 1)
    column = lane & (NB - 1)
    chunks = []
    spill = jnp.zeros((ROWS, 128), F32)
    for q in range(16):
        low = read(q)
        high = read(31 - q)
        if weigh:
            low = jnp.where((column >> 1) == q, low * 0.5, low)
        turned = pltpu.roll(high, 2 * q, 1) if q else high
        chunks.append(jnp.where(column >= 2 * q, low, turned))
        block = (column >> 1) == (31 - q)
        spill = jnp.where(block, high * 0.5 if weigh else high, spill)
    return chunks, spill


def pack_kernel(a_ref, p_ref, slot_ref, touched_ref, out_ref):
    r = iota((ROWS, ROWS), 0)
    c = iota((ROWS, ROWS), 1)

    def as_column(row):
        return jnp.sum(jnp.where(r == c, row, 0.0), axis=1, keepdims=True)

    slot = slot_ref[...]
    owner_row = (slot >> 6).astype(F32)
    inner_row = (slot & (ROWS - 1)).astype(F32)
    touched_row = touched_ref[...].astype(F32)
    owner_full = jnp.broadcast_to(owner_row, (ROWS, ROWS))
    owner_col = as_column(owner_full)
    inner_col = as_column(jnp.broadcast_to(inner_row, (ROWS, ROWS)))
    touched_col = as_column(jnp.broadcast_to(touched_row, (ROWS, ROWS)))
    rank = jnp.sum(ones_where((owner_col == owner_full) & (r < c)), axis=0, keepdims=True)
    lower = jnp.sum(ones_where(owner_col < owner_full), axis=0, keepdims=True)
    place = rank * 16.0 + lower * 0.25
    select = ones_where(r.astype(F32) == place, BF16)
    lane = iota((ROWS, 128), 1)

    def with_ids(spill, first):
        ids = jnp.where(lane == first, touched_col, jnp.where(lane == first + 1, owner_col, inner_col))
        return jnp.where((lane & (NB - 1)) >= 32, spill, jnp.where((lane >= first) & (lane < first + 3), ids, 0.0))

    chunks, spill = folded(lambda q: a_ref[:, q * 128 : (q + 1) * 128].astype(F32), False)
    chunks.append(with_ids(spill, 0))
    for q, chunk in enumerate(chunks):
        picked = nn(select, chunk.astype(BF16)).astype(BF16)
        for k in range(SIDE):
            out_ref[k, 0:16, q * 128 : (q + 1) * 128] = picked[16 * k : 16 * (k + 1)]
    chunks, spill = folded(lambda q: p_ref[:, q * 128 : (q + 1) * 128].astype(F32), True)
    chunks.append(with_ids(spill, 3))
    for q, chunk in enumerate(chunks):
        rounded = chunk.astype(BF16)
        for k in range(SIDE):
            out_ref[k, 16:80, q * 128 : (q + 1) * 128] = rounded


def score_kernel(core_ref, rows_ref, near_ref, far_ref, out_ref, col_ref, row_ref):
    n_rows, n_cols = 256, 512
    rows = jnp.concatenate([rows_ref[k, 16:80, :] for k in range(SIDE)], axis=0)
    near = near_ref[...].reshape(256, WIDTH)
    far = far_ref[...].reshape(256, WIDTH)
    scores = jnp.concatenate([nt(near, rows), nt(far, rows)], axis=0)
    last = slice(16 * 128, WIDTH)
    col_ids = jnp.concatenate([near[:, last], far[:, last]], axis=0)
    row_ids = rows[:, last]
    pick = iota((8, 128), 0)
    spot = iota((8, 128), 1)
    col_t = nt(ones_where(pick == spot, BF16), col_ids)
    row_t = nt(ones_where(pick + 3 == spot, BF16), row_ids)
    lane_c = iota((n_cols, 128), 1).astype(F32)
    lane_r = iota((n_rows, 128), 1).astype(F32)
    col_f = col_ids.astype(F32)
    row_f = row_ids.astype(F32)
    kind_c = ones_where(col_f[:, 0:1] == lane_c, BF16)
    kind_r = ones_where(row_f[:, 3:4] == lane_r, BF16)
    same_kind = nt(kind_c, kind_r)
    scores = jnp.where(same_kind > 0.5, scores, 0.0)
    own_c = ones_where(col_f[:, 1:2] == lane_c, BF16)
    i = iota((n_cols, n_cols), 0)
    j = iota((n_cols, n_cols), 1)
    same = nt(own_c, own_c)
    turn = core_ref[0] * 256
    rank_c = jnp.sum(jnp.where((i ^ turn) < (j ^ turn), same, 0.0), axis=0, keepdims=True)
    place = col_t[1:2, :] * 16.0 + rank_c
    move = ones_where(i.astype(F32) == place)
    out_ref[...] = nn(move, scores, HI).astype(out_ref.dtype)
    odd = col_t[1:2, :] - 2.0 * jnp.floor(col_t[1:2, :] * 0.5)
    col_id = odd * 64.0 + col_t[2:3, :]
    col_ref[...] = nt(jnp.broadcast_to(col_id, (8, n_cols)), move, HI)
    own_r = ones_where(row_f[:, 4:5] == lane_r, BF16)
    ri = iota((n_rows, n_rows), 0)
    rj = iota((n_rows, n_rows), 1)
    same_r = nt(own_r, own_r)
    rank_r = jnp.sum(jnp.where((ri < rj) & ((ri >> 6) == (rj >> 6)), same_r, 0.0), axis=0, keepdims=True)
    line = (iota((1, n_rows), 1) >> 6).astype(F32)
    row_ref[0:1, :] = row_t[1:2, :] * 8.0 + line
    row_ref[1:2, :] = rank_r
    row_ref[2:3, :] = row_t[2:3, :] + 1.0
    row_ref[3:8, :] = jnp.zeros((5, n_rows), F32)


def send_kernel(group_ref, z_ref, col_ref, row_ref, out_ref):
    total = z_ref[0].astype(F32)
    for g in range(1, z_ref.shape[0]):
        total = total + z_ref[g].astype(F32)
    m = iota((256, 256), 0).astype(F32)
    target = row_ref[0:1, :]
    rank = row_ref[1:2, :]
    inner = jnp.broadcast_to(row_ref[2:3, :], (8, 256))
    s = iota((512, 128), 0)
    lane = iota((512, 128), 1)
    here = ones_where(s == group_ref[0] * 32 + (lane & 31))
    cols = nn(col_ref[...], here, HI)[0:1, :]
    values, indices = [], []
    for k in range(SIDE):
        values.append(nt(ones_where((m == target) & (rank == float(k))), total, HI))
        found = nt(ones_where((m == target + 4.0) & (rank == float(k))), inner, HI)
        indices.append(jnp.broadcast_to(found[:, 0:1], (256, 32)))
    value = jnp.concatenate(values, axis=1)
    index = jnp.concatenate(indices, axis=1) * 128.0 + cols
    is_id = (iota((256, 128), 0) & 7) >= 4
    out_ref[...] = jnp.where(is_id, index, value)


def land_kernel(in_ref, out_ref):
    parts = [in_ref[64 * x : 64 * (x + 1), :] for x in range(SIDE)]
    lane = iota((64, 512), 1)
    wide = jnp.concatenate(parts, axis=1)
    index = parts[0]
    high = jnp.floor(index * (1.0 / 128.0))
    high = pltpu.roll(high, 60, 0)
    is_value = (iota((64, 64), 0) & 7) < 4
    spot = iota((64, 64), 1).astype(F32) + 1.0
    total = None
    for k in range(SIDE):
        place = ones_where(is_value & (high[:, 32 * k : 32 * k + 1] == spot))
        part = tn(place, jnp.where(((lane >> 5) & 3) == k, wide, 0.0), HI)
        total = part if total is None else total + part
    id_row = wide[4:5, :]
    col = id_row - 128.0 * jnp.floor(id_row * (1.0 / 128.0))
    spread = ones_where(iota((128, 512), 0).astype(F32) == col)
    out_ref[...] = nt(total, spread, HI)


def call(kernel, out, n, first=VMEM):
    many = isinstance(out, tuple)
    return pl.pallas_call(
        kernel,
        out_shape=out,
        in_specs=[first] + [VMEM] * (n - 1),
        out_specs=tuple(VMEM for _ in out) if many else VMEM,
    )


def masked_blocks(blocks, block_class):
    block_order = blocks.shape[1]
    positions = jnp.arange(block_order)
    active = block_order // 2 * (1 + block_class)
    inside = (positions[None, :, None] < active[:, None, None]) & (
        positions[None, None, :] < active[:, None, None]
    )
    return jnp.where(inside, blocks, jnp.zeros_like(blocks))


def device(x, y, c):
    return (x * SIDE + y) * 2 + c


LINES_X = [[device(x, y, c) for x in range(SIDE)] for y in range(SIDE) for c in range(2)]
LINES_Y = [[device(x, y, c) for y in range(SIDE)] for x in range(SIDE) for c in range(2)]
SWAP = [(device(x, y, c), device(x, y, 1 - c)) for x in range(SIDE) for y in range(SIDE) for c in range(2)]


def shards(a_pieces, touched, slot_row, x_blocks, z_inverse, block_class):
    x_masked = masked_blocks(x_blocks, block_class)
    z_masked = masked_blocks(z_inverse, block_class)
    own_block = touched[0]
    a_local = a_pieces[0]
    pieces = a_local.reshape(ROWS, NB, NB)
    left = jnp.einsum("rab,rbc->rac", x_masked[own_block], pieces, preferred_element_type=F32).astype(BF16)
    product = jnp.einsum("rab,rbc->rac", left, z_masked[own_block], preferred_element_type=F32)
    both = (product + jnp.swapaxes(product, 1, 2)).astype(BF16).reshape(ROWS, NB * NB)
    packed = call(pack_kernel, jax.ShapeDtypeStruct((SIDE, DEPTH, WIDTH), BF16), 4)(
        a_local, both, slot_row[None, :], touched
    )
    lined = lax.all_to_all(packed, "row", 0, 0, tiled=True, axis_index_groups=LINES_X)
    mine = lined[:, :16, :].reshape(ROWS, WIDTH)
    near = lax.all_to_all(
        jnp.broadcast_to(mine[None], (SIDE, ROWS, WIDTH)), "row", 0, 0, tiled=True, axis_index_groups=LINES_Y
    )
    far = lax.ppermute(near, "row", SWAP)
    core = (lax.axis_index("row").astype(jnp.int32) & 1).reshape(1)
    scores, cols, rows = call(
        score_kernel,
        (
            jax.ShapeDtypeStruct((512, 256), Z_TYPE),
            jax.ShapeDtypeStruct((8, 512), F32),
            jax.ShapeDtypeStruct((8, 256), F32),
        ),
        4,
        SMEM,
    )(core, lined, near, far)
    summed = lax.all_to_all(scores.reshape(16, 32, 256), "grp", 0, 0, tiled=True)
    group = lax.axis_index("grp").astype(jnp.int32).reshape(1)
    outgoing = call(send_kernel, jax.ShapeDtypeStruct((256, 128), F32), 4, SMEM)(group, summed, cols, rows)
    incoming = lax.all_to_all(outgoing.reshape(32, 8, 128), "row", 0, 0, tiled=True)
    return call(land_kernel, jax.ShapeDtypeStruct((64, 128), F32), 1)(incoming.reshape(256, 128))


def solution(mesh):
    return jax.shard_map(
        shards,
        mesh=mesh,
        in_specs=(
            P("grp", "row", None),
            P("grp", "row"),
            P("row"),
            P("grp", None, None),
            P("grp", None, None),
            P("grp"),
        ),
        out_specs=P("row", "grp"),
        check_vma=False,
    )
```

```python
import jax
import jax.numpy as jnp
from jax import lax
from jax.experimental import pallas as pl
from jax.experimental.pallas import tpu as pltpu
from jax.sharding import PartitionSpec as P

F32 = jnp.float32
BF16 = jnp.bfloat16
NB = 64
CHUNKS = 17
WIDTH = CHUNKS * 128
ROWS = 64
SIDE = 4
DEPTH = 80
SLAB = 72
PAIRS = 16
VMEM = pl.BlockSpec(memory_space=pltpu.VMEM)
SMEM = pl.BlockSpec(memory_space=pltpu.SMEM)


def iota(shape, dim):
    return lax.broadcasted_iota(jnp.int32, shape, dim)


def ones_where(cond, dtype=F32):
    return jnp.where(cond, 1.0, 0.0).astype(dtype)


def nt(a, b, precision=None):
    return lax.dot_general(a, b, (((1,), (1,)), ((), ())), precision=precision, preferred_element_type=F32)


def tn(a, b, precision=None):
    return lax.dot_general(a, b, (((0,), (0,)), ((), ())), precision=precision, preferred_element_type=F32)


def nn(a, b, precision=None):
    return lax.dot_general(a, b, (((1,), (0,)), ((), ())), precision=precision, preferred_element_type=F32)


def thirds(x):
    high = x.astype(BF16)
    rest = x - high.astype(F32)
    middle = rest.astype(BF16)
    return high, middle, (rest - middle.astype(F32)).astype(BF16)


def folded(read, weigh):
    lane = iota((ROWS, 128), 1)
    column = lane & (NB - 1)
    chunks = []
    spill = jnp.zeros((ROWS, 128), F32)
    for q in range(16):
        low = read(q)
        high = read(31 - q)
        if weigh:
            low = jnp.where((column >> 1) == q, low * 0.5, low)
        turned = pltpu.roll(high, 2 * q, 1) if q else high
        chunks.append(jnp.where(column >= 2 * q, low, turned))
        block = (column >> 1) == (31 - q)
        spill = jnp.where(block, high * 0.5 if weigh else high, spill)
    return chunks, spill


def products(kind_ref, class_ref, x_ref, z_ref, tile_ref, both_ref, left_ref, right_ref, turned_ref):
    s = iota((NB, NB), 0)
    turn = ones_where(iota((NB, NB), 1) == ((s & 31) * 2 + (s >> 5)), BF16)
    rr = iota((NB, NB), 0)
    cc = iota((NB, NB), 1)
    empty = jnp.zeros((NB, NB), BF16)

    def beside(u, v):
        return jnp.concatenate([u, v], axis=1)

    for k in range(x_ref.shape[0]):
        active = (NB // 2) * (1 + class_ref[k])
        inside = (rr < active) & (cc < active)
        x = jnp.where(inside, x_ref[k].astype(F32), 0.0).astype(BF16)
        z = jnp.where(inside, z_ref[k].astype(F32), 0.0).astype(BF16)
        half = nt(x, turn).astype(BF16)
        full = nn(turn, half).astype(BF16)
        left_ref[k, 0:NB, :] = beside(full, full)
        left_ref[k, NB : 2 * NB, :] = beside(half, half)
        right_ref[k, 0:NB, :] = beside(z, empty)
        right_ref[k, NB : 2 * NB, :] = beside(empty, z)
        back = nn(turn, z).astype(BF16)
        turned_ref[k] = beside(back, back)

    def first(rows):
        return iota((rows, 128), 1) < NB

    def split(v):
        none = jnp.zeros_like(v)
        low = first(v.shape[0])
        return jnp.concatenate([jnp.where(low, v, none), jnp.where(low, none, v)], axis=0)

    def step(outer, carry):
        for inner in range(PAIRS):
            i = (outer * PAIRS + inner) * 2
            k0 = kind_ref[0, i]
            k1 = kind_ref[0, i + 1]
            at0 = pl.ds(pl.multiple_of(i * 32, 32), 32)
            at1 = pl.ds(pl.multiple_of(i * 32 + 32, 32), 32)
            tile0 = tile_ref[pl.ds(i, 32, stride=ROWS), :]
            tile1 = tile_ref[pl.ds(i + 1, 32, stride=ROWS), :]
            low = first(32)
            top = jnp.where(low, tile0, pltpu.roll(tile1, NB, 1))
            bottom = jnp.where(low, pltpu.roll(tile0, NB, 1), tile1)
            pieces = split(jnp.concatenate([top, bottom], axis=0)).astype(BF16)
            left = nn(jnp.where(first(2 * NB), left_ref[k0], left_ref[k1]), pieces)
            right = jnp.concatenate([right_ref[k0, 0:NB, :], right_ref[k1, NB : 2 * NB, :]], axis=0)
            turned = jnp.where(first(NB), turned_ref[k0], turned_ref[k1])
            both = nn(left[:NB].astype(BF16), right) + nt(turned, split(left[NB:]).astype(BF16))
            top = both[:32]
            bottom = both[32:]
            both_ref[at0, :] = jnp.where(low, top, pltpu.roll(bottom, NB, 1))
            both_ref[at1, :] = jnp.where(low, pltpu.roll(top, NB, 1), bottom)
        return carry

    lax.fori_loop(0, ROWS // (2 * PAIRS), step, 0)


def pack_kernel(
    kind_ref, class_ref, a_ref, x_ref, z_ref, slot_ref, touched_ref, out_ref, tile_ref, both_ref, left_ref, right_ref, turned_ref
):
    for q in range(32):
        tile_ref[q * ROWS : (q + 1) * ROWS, :] = a_ref[:, q * 128 : (q + 1) * 128].astype(F32)
    products(kind_ref, class_ref, x_ref, z_ref, tile_ref, both_ref, left_ref, right_ref, turned_ref)
    r = iota((ROWS, ROWS), 0)
    c = iota((ROWS, ROWS), 1)

    def as_column(row):
        return jnp.sum(jnp.where(r == c, row, 0.0), axis=1, keepdims=True)

    slot = slot_ref[...]
    owner_row = (slot >> 6).astype(F32)
    inner_row = (slot & (ROWS - 1)).astype(F32)
    touched_row = touched_ref[...].astype(F32)
    owner_full = jnp.broadcast_to(owner_row, (ROWS, ROWS))
    owner_col = as_column(owner_full)
    inner_col = as_column(jnp.broadcast_to(inner_row, (ROWS, ROWS)))
    touched_col = as_column(jnp.broadcast_to(touched_row, (ROWS, ROWS)))
    rank = jnp.sum(ones_where((owner_col == owner_full) & (r < c)), axis=0, keepdims=True)
    lower = jnp.sum(ones_where(owner_col < owner_full), axis=0, keepdims=True)
    place = rank * 16.0 + lower * 0.25
    select = ones_where(r.astype(F32) == place, BF16)
    lane = iota((ROWS, 128), 1)

    def with_ids(spill, first):
        ids = jnp.where(lane == first, touched_col, jnp.where(lane == first + 1, owner_col, inner_col))
        return jnp.where((lane & (NB - 1)) >= 32, spill, jnp.where((lane >= first) & (lane < first + 3), ids, 0.0))

    chunks, spill = folded(lambda q: a_ref[:, q * 128 : (q + 1) * 128].astype(F32), False)
    chunks.append(with_ids(spill, 0))
    for q, chunk in enumerate(chunks):
        picked = nn(select, chunk.astype(BF16)).astype(BF16)
        for k in range(SIDE):
            out_ref[k, 0:16, q * 128 : (q + 1) * 128] = picked[16 * k : 16 * (k + 1)]
    chunks, spill = folded(lambda q: both_ref[pl.ds(q, ROWS, stride=32), :], True)
    chunks.append(with_ids(spill, 3))
    for q, chunk in enumerate(chunks):
        rounded = chunk.astype(BF16)
        for k in range(SIDE):
            out_ref[k, 16:80, q * 128 : (q + 1) * 128] = rounded


def near_kernel(rows_ref, near_ref, score_ref, col_id_ref, row_id_ref, row_ref):
    rows = jnp.concatenate([rows_ref[k, 16:80, :] for k in range(SIDE)], axis=0)
    near = near_ref[...].reshape(256, WIDTH)
    score_ref[...] = nt(near, rows)
    row_ids = rows[:, 16 * 128 :]
    col_id_ref[...] = near[:, 16 * 128 :]
    row_id_ref[...] = row_ids
    row_t = nt(ones_where(iota((8, 128), 0) + 3 == iota((8, 128), 1), BF16), row_ids)
    lane = iota((256, 128), 1).astype(F32)
    own = ones_where(row_ids.astype(F32)[:, 4:5] == lane, BF16)
    i = iota((256, 256), 0)
    j = iota((256, 256), 1)
    rank = jnp.sum(jnp.where((i < j) & ((i >> 6) == (j >> 6)), nt(own, own), 0.0), axis=0, keepdims=True)
    line = (iota((1, 256), 1) >> 6).astype(F32)
    row_ref[0:1, :] = row_t[1:2, :] * 8.0 + line
    row_ref[1:2, :] = rank
    row_ref[2:3, :] = row_t[2:3, :] + 1.0
    row_ref[3:8, :] = jnp.zeros((5, 256), F32)


def score_kernel(core_ref, rows_ref, far_ref, score_ref, col_id_ref, row_id_ref, out_ref, col_ref):
    n_rows, n_cols = 256, 512
    rows = jnp.concatenate([rows_ref[k, 16:80, :] for k in range(SIDE)], axis=0)
    far = far_ref[...].reshape(256, WIDTH)
    scores = jnp.concatenate([score_ref[...], nt(far, rows)], axis=0)
    col_ids = jnp.concatenate([col_id_ref[...], far[:, 16 * 128 :]], axis=0)
    col_t = nt(ones_where(iota((8, 128), 0) == iota((8, 128), 1), BF16), col_ids)
    lane_c = iota((n_cols, 128), 1).astype(F32)
    lane_r = iota((n_rows, 128), 1).astype(F32)
    col_f = col_ids.astype(F32)
    kind_c = ones_where(col_f[:, 0:1] == lane_c, BF16)
    kind_r = ones_where(row_id_ref[...].astype(F32)[:, 3:4] == lane_r, BF16)
    scores = jnp.where(nt(kind_c, kind_r) > 0.5, scores, 0.0)
    own_c = ones_where(col_f[:, 1:2] == lane_c, BF16)
    i = iota((n_cols, n_cols), 0)
    j = iota((n_cols, n_cols), 1)
    turn = core_ref[0] * 256
    rank = jnp.sum(jnp.where((i ^ turn) < (j ^ turn), nt(own_c, own_c), 0.0), axis=0, keepdims=True)
    move = ones_where(i.astype(F32) == col_t[1:2, :] * 16.0 + rank, BF16)
    top = jnp.max(jnp.max(jnp.abs(scores), axis=0, keepdims=True), axis=1, keepdims=True)
    power = jnp.ceil(jnp.log(jnp.maximum(top, 1e-36)) * 1.4426950408889634)
    scaled = scores * jnp.exp2(-power)
    high = scaled.astype(BF16)
    low = (scaled - high.astype(F32)).astype(BF16)
    moved = nn(move, high) + nn(move, low)
    note = jnp.broadcast_to(power, (8, 128))
    for g in range(16):
        out_ref[g, 0:32, :] = moved[32 * g : 32 * (g + 1), 0:128]
        out_ref[g, 32:64, :] = moved[32 * g : 32 * (g + 1), 128:256]
        out_ref[g, 64:72, :] = note
    odd = col_t[1:2, :] - 2.0 * jnp.floor(col_t[1:2, :] * 0.5)
    col_id = (odd * 64.0 + col_t[2:3, :]).astype(BF16)
    col_ref[...] = nt(jnp.broadcast_to(col_id, (8, n_cols)), move)


def send_kernel(group_ref, total_ref, col_ref, row_ref, out_ref):
    total = jnp.concatenate([total_ref[0:32, :], total_ref[32:64, :]], axis=1)
    target = row_ref[0:1, :]
    rank = row_ref[1:2, :]
    m = iota((256, 256), 0).astype(F32)
    hit = (m == target) | (m == target + 4.0)
    pick = jnp.concatenate([ones_where(hit & (rank == float(k)), BF16) for k in range(SIDE)], axis=0)
    high, middle, low = thirds(total)
    inner = jnp.broadcast_to(row_ref[2:3, :], (16, 256)).astype(BF16)
    found = nt(pick, jnp.concatenate([high, inner], axis=0))
    value = found[:, 0:32] + (nt(pick, middle) + nt(pick, low))
    index = jnp.broadcast_to(found[:, 32:33], (4 * 256, 32))
    s = iota((512, 128), 0)
    lane = iota((512, 128), 1)
    here = ones_where(s == group_ref[0] * 32 + (lane & 31), BF16)
    cols = nn(col_ref[...].astype(BF16), here)[0:1, :]
    values = jnp.concatenate([value[256 * k : 256 * (k + 1)] for k in range(SIDE)], axis=1)
    indices = jnp.concatenate([index[256 * k : 256 * (k + 1)] for k in range(SIDE)], axis=1)
    is_id = (iota((256, 128), 0) & 7) >= 4
    out_ref[...] = jnp.where(is_id, indices * 128.0 + cols, values)


def land_kernel(in_ref, out_ref):
    wide = jnp.concatenate([in_ref[64 * x : 64 * (x + 1), :] for x in range(SIDE)], axis=1)
    lane = (iota((64, 512), 1) >> 5) & 3
    index = in_ref[0:64, :]
    high = pltpu.roll(jnp.floor(index * (1.0 / 128.0)), 60, 0)
    is_value = (iota((64, 64), 0) & 7) < 4
    spot = iota((64, 64), 1).astype(F32) + 1.0
    place = jnp.concatenate(
        [ones_where(is_value & (high[:, 32 * k : 32 * k + 1] == spot), BF16) for k in range(SIDE)], axis=0
    )
    own = [jnp.where(lane == k, wide, 0.0) for k in range(SIDE)]
    total = None
    for part in thirds(jnp.concatenate(own, axis=0)):
        term = tn(place, part)
        total = term if total is None else total + term
    id_row = wide[4:5, :]
    col = id_row - 128.0 * jnp.floor(id_row * (1.0 / 128.0))
    spread = ones_where(iota((128, 512), 0).astype(F32) == col, BF16)
    high, middle, low = thirds(total)
    out_ref[...] = nt(high, spread) + (nt(middle, spread) + nt(low, spread))


def near_by(*dims, dtype=F32):
    return pltpu.VMEM(dims, dtype)


def shape(*dims, dtype=F32):
    return jax.ShapeDtypeStruct(dims, dtype)


def call(kernel, out, n, scalars=0, scratch=(), held=()):
    many = isinstance(out, tuple)
    run = pl.pallas_call(
        kernel,
        out_shape=out,
        in_specs=[SMEM] * scalars + [VMEM] * (n - scalars),
        out_specs=tuple(VMEM for _ in out) if many else VMEM,
        scratch_shapes=list(scratch),
    )

    def placed(*args):
        return run(
            *(pltpu.with_memory_space_constraint(a, pltpu.VMEM) if i in held else a for i, a in enumerate(args))
        )

    return placed


def device(x, y, c):
    return (x * SIDE + y) * 2 + c


LINES_X = [[device(x, y, c) for x in range(SIDE)] for y in range(SIDE) for c in range(2)]
LINES_Y = [[device(x, y, c) for y in range(SIDE)] for x in range(SIDE) for c in range(2)]
SWAP = [(device(x, y, c), device(x, y, 1 - c)) for x in range(SIDE) for y in range(SIDE) for c in range(2)]


def shards(a_pieces, touched, slot_row, x_blocks, z_inverse, block_class):
    blocks = x_blocks.shape[0]
    packed = call(
        pack_kernel,
        near_by(SIDE, DEPTH, WIDTH, dtype=BF16),
        7,
        2,
        (
            pltpu.VMEM((ROWS * 32, 128), F32),
            pltpu.VMEM((ROWS * 32, 128), F32),
            pltpu.VMEM((blocks, 2 * NB, 2 * NB), BF16),
            pltpu.VMEM((blocks, 2 * NB, 2 * NB), BF16),
            pltpu.VMEM((blocks, NB, 2 * NB), BF16),
        ),
    )(touched, block_class, a_pieces[0], x_blocks, z_inverse, slot_row[None, :], touched)
    lined = lax.all_to_all(packed, "row", 0, 0, tiled=True, axis_index_groups=LINES_X)
    mine = lined[:, :16, :].reshape(ROWS, WIDTH)
    near = lax.all_to_all(
        jnp.broadcast_to(mine[None], (SIDE, ROWS, WIDTH)), "row", 0, 0, tiled=True, axis_index_groups=LINES_Y
    )
    far = lax.ppermute(near, "row", SWAP)
    near_scores, col_ids, row_ids, rows = call(
        near_kernel, (shape(256, 256), shape(256, 128, dtype=BF16), shape(256, 128, dtype=BF16), shape(8, 256)), 2
    )(lined, near)
    core = (lax.axis_index("row").astype(jnp.int32) & 1).reshape(1)
    scores, cols = call(score_kernel, (near_by(16, SLAB, 128), near_by(8, 512)), 6, 1, held=())(
        core, lined, far, near_scores, col_ids, row_ids
    )
    group = lax.axis_index("grp").astype(jnp.int32).reshape(1)
    sent, cols, rows, group = lax.optimization_barrier((scores.astype(jnp.float16), cols, rows, group))
    arrived = lax.all_to_all(sent, "grp", 0, 0, tiled=True).astype(F32)
    total = jnp.sum(arrived[:, :64] * jnp.exp2(arrived[:, 64:65]), axis=0)
    outgoing = call(send_kernel, near_by(256, 128), 4, 1, held=(1, 2))(group, total, cols, rows)
    incoming = lax.all_to_all(outgoing.reshape(32, 8, 128), "row", 0, 0, tiled=True)
    return call(land_kernel, shape(64, 128), 1, held=(0,))(incoming.reshape(256, 128))


def solution(mesh):
    return jax.shard_map(
        shards,
        mesh=mesh,
        in_specs=(
            P("grp", "row", None),
            P("grp", "row"),
            P("row"),
            P("grp", None, None),
            P("grp", None, None),
            P("grp"),
        ),
        out_specs=P("row", "grp"),
        check_vma=False,
    )
```

```python
import jax
import jax.numpy as jnp
from jax import lax
from jax.experimental import pallas as pl
from jax.experimental.pallas import tpu as pltpu
from jax.sharding import PartitionSpec as P

F32 = jnp.float32
BF16 = jnp.bfloat16
NB = 64
CHUNKS = 17
WIDTH = CHUNKS * 128
ROWS = 64
SIDE = 4
SLAB = 72
QUADS = 8
GRANT = 16 << 20
WIDE = 60 << 20
VMEM = pl.BlockSpec(memory_space=pltpu.VMEM)
SMEM = pl.BlockSpec(memory_space=pltpu.SMEM)


def iota(shape, dim):
    return lax.broadcasted_iota(jnp.int32, shape, dim)


def ones_where(cond, dtype=F32):
    return jnp.where(cond, 1.0, 0.0).astype(dtype)


def nt(a, b, precision=None):
    return lax.dot_general(a, b, (((1,), (1,)), ((), ())), precision=precision, preferred_element_type=F32)


def tn(a, b, precision=None):
    return lax.dot_general(a, b, (((0,), (0,)), ((), ())), precision=precision, preferred_element_type=F32)


def nn(a, b, precision=None):
    return lax.dot_general(a, b, (((1,), (0,)), ((), ())), precision=precision, preferred_element_type=F32)


def thirds(x):
    high = x.astype(BF16)
    rest = x - high.astype(F32)
    middle = rest.astype(BF16)
    return high, middle, (rest - middle.astype(F32)).astype(BF16)


def folded(read, weigh):
    lane = iota((ROWS, 128), 1)
    column = lane & (NB - 1)
    chunks = []
    spill = jnp.zeros((ROWS, 128), F32)
    for q in range(16):
        low = read(q)
        high = read(31 - q)
        if weigh:
            low = jnp.where((column >> 1) == q, low * 0.5, low)
        turned = pltpu.roll(high, 2 * q, 1) if q else high
        chunks.append(jnp.where(column >= 2 * q, low, turned))
        block = (column >> 1) == (31 - q)
        spill = jnp.where(block, high * 0.5 if weigh else high, spill)
    return chunks, spill


def products(kind_ref, class_ref, x_ref, z_ref, tile_ref, both_ref, left_ref, right_ref, turned_ref):
    s = iota((NB, NB), 0)
    turn = ones_where(iota((NB, NB), 1) == ((s & 31) * 2 + (s >> 5)), BF16)
    rr = iota((NB, NB), 0)
    cc = iota((NB, NB), 1)
    empty = jnp.zeros((NB, NB), BF16)

    def beside(u, v):
        return jnp.concatenate([u, v], axis=1)

    for k in range(x_ref.shape[0]):
        active = (NB // 2) * (1 + class_ref[k])
        inside = (rr < active) & (cc < active)
        x = jnp.where(inside, x_ref[k].astype(F32), 0.0).astype(BF16)
        z = jnp.where(inside, z_ref[k].astype(F32), 0.0).astype(BF16)
        half = nt(x, turn).astype(BF16)
        full = nn(turn, half).astype(BF16)
        left_ref[k, 0:NB, :] = beside(full, full)
        left_ref[k, NB : 2 * NB, :] = beside(half, half)
        right_ref[k, 0:NB, :] = beside(z, empty)
        right_ref[k, NB : 2 * NB, :] = beside(empty, z)
        back = nn(turn, z).astype(BF16)
        turned_ref[k] = beside(back, back)

    def first(rows):
        return iota((rows, 128), 1) < NB

    def split(v):
        none = jnp.zeros_like(v)
        low = first(v.shape[0])
        return jnp.concatenate([jnp.where(low, v, none), jnp.where(low, none, v)], axis=0)

    def corners(u, v):
        none = jnp.zeros_like(u)
        return jnp.concatenate([beside(u, none), beside(none, v)], axis=0)

    def step(outer, carry):
        low = first(32)
        for inner in range(QUADS):
            i = (outer * QUADS + inner) * 4
            k = [kind_ref[0, i + n] for n in range(4)]
            cats, lefts, rights, backs = [], [], [], []
            for p in (0, 2):
                tile0 = tile_ref[pl.ds(i + p, 32, stride=ROWS), :]
                tile1 = tile_ref[pl.ds(i + p + 1, 32, stride=ROWS), :]
                top = jnp.where(low, tile0, pltpu.roll(tile1, NB, 1))
                bottom = jnp.where(low, pltpu.roll(tile0, NB, 1), tile1)
                cats.append(split(jnp.concatenate([top, bottom], axis=0)).astype(BF16))
                lefts.append(jnp.where(first(2 * NB), left_ref[k[p]], left_ref[k[p + 1]]))
                rights.append(
                    jnp.concatenate([right_ref[k[p], 0:NB, :], right_ref[k[p + 1], NB : 2 * NB, :]], axis=0)
                )
                backs.append(jnp.where(first(NB), turned_ref[k[p]], turned_ref[k[p + 1]]))
            left = nn(beside(*lefts), corners(*cats))
            halves = [split(left[NB:, 128 * p : 128 * (p + 1)]).astype(BF16) for p in range(2)]
            both = nn(left[:NB].astype(BF16), corners(*rights)) + nt(beside(*backs), corners(*halves))
            for p in range(2):
                top = both[:32, 128 * p : 128 * (p + 1)]
                bottom = both[32:, 128 * p : 128 * (p + 1)]
                at = pl.multiple_of((i + 2 * p) * 32, 64)
                both_ref[pl.ds(at, 32), :] = jnp.where(low, top, pltpu.roll(bottom, NB, 1))
                both_ref[pl.ds(at + 32, 32), :] = jnp.where(low, pltpu.roll(top, NB, 1), bottom)
        return carry

    lax.fori_loop(0, ROWS // (4 * QUADS), step, 0)


def slot_table(me_ref, slot_ref, touched_ref):
    r = iota((ROWS, ROWS), 0)
    c = iota((ROWS, ROWS), 1)

    def spread(row):
        full = jnp.broadcast_to(row, (ROWS, ROWS))
        return full, jnp.sum(jnp.where(r == c, full, 0.0), axis=1, keepdims=True)

    slot = slot_ref[...]
    owner_full, owner_col = spread((slot >> 6).astype(F32))
    _, inner_col = spread((slot & (ROWS - 1)).astype(F32))
    _, touched_col = spread(touched_ref[...].astype(F32))
    rank = jnp.sum(ones_where((owner_col == owner_full) & (r < c)), axis=0, keepdims=True)
    lower = jnp.sum(ones_where(owner_col < owner_full), axis=0, keepdims=True)
    holder = jnp.full((ROWS, 1), me_ref[0], jnp.int32).astype(F32)
    return (touched_col, owner_col, inner_col, holder), rank * 16.0 + lower * 0.25


def with_ids(spill, columns, first):
    lane = iota((ROWS, 128), 1)
    ids = jnp.zeros((ROWS, 128), F32)
    for n, column in enumerate(columns):
        ids = jnp.where(lane == first + n, column, ids)
    return jnp.where((lane & (NB - 1)) >= 32, spill, ids)


def pack_kernel(me_ref, a_ref, slot_ref, touched_ref, out_ref):
    columns, place = slot_table(me_ref, slot_ref, touched_ref)
    select = ones_where(iota((ROWS, ROWS), 0).astype(F32) == place, BF16)
    chunks, spill = folded(lambda q: a_ref[:, q * 128 : (q + 1) * 128].astype(F32), False)
    chunks.append(with_ids(spill, columns, 0))
    for q, chunk in enumerate(chunks):
        picked = nn(select, chunk.astype(BF16)).astype(BF16)
        for k in range(SIDE):
            out_ref[k, :, q * 128 : (q + 1) * 128] = picked[16 * k : 16 * (k + 1)]


def product_kernel(
    me_ref, kind_ref, class_ref, a_ref, x_ref, z_ref, slot_ref, touched_ref, out_ref, tile_ref, both_ref, left_ref, right_ref, turned_ref
):
    for q in range(32):
        tile_ref[q * ROWS : (q + 1) * ROWS, :] = a_ref[:, q * 128 : (q + 1) * 128].astype(F32)
    products(kind_ref, class_ref, x_ref, z_ref, tile_ref, both_ref, left_ref, right_ref, turned_ref)
    columns, _ = slot_table(me_ref, slot_ref, touched_ref)
    chunks, spill = folded(lambda q: both_ref[pl.ds(q, ROWS, stride=32), :], True)
    chunks.append(with_ids(spill, columns, 4))
    for q, chunk in enumerate(chunks):
        rounded = chunk.astype(BF16)
        for k in range(SIDE):
            out_ref[k, :, q * 128 : (q + 1) * 128] = rounded


def score_kernel(rows_ref, near_ref, far_ref, out_ref, col_ref, row_ref):
    n_rows, n_cols = 256, 512
    rows = rows_ref[...].reshape(n_rows, WIDTH)
    near = near_ref[...].reshape(256, WIDTH)
    far = far_ref[...].reshape(256, WIDTH)
    scores = jnp.concatenate([nt(near, rows), nt(far, rows)], axis=0)
    col_ids = jnp.concatenate([near[:, 16 * 128 :], far[:, 16 * 128 :]], axis=0)
    row_ids = rows[:, 16 * 128 :]
    pick = iota((8, 128), 0)
    spot = iota((8, 128), 1)
    col_t = nt(ones_where(pick == spot, BF16), col_ids)
    row_t = nt(ones_where(pick + 4 == spot, BF16), row_ids)
    col_f = col_ids.astype(F32)
    row_f = row_ids.astype(F32)
    lane_r = iota((n_rows, 128), 1).astype(F32)
    own_r = ones_where(row_f[:, 5:6] == lane_r, BF16)
    before = (iota((n_rows, n_rows), 0) < iota((n_rows, n_rows), 1)) & (row_f[:, 7:8] == row_t[3:4, :])
    row_rank = jnp.sum(jnp.where(before, nt(own_r, own_r), 0.0), axis=0, keepdims=True)
    row_ref[0:1, :] = row_t[1:2, :] * 8.0 + jnp.floor(row_t[3:4, :] * 0.125)
    row_ref[1:2, :] = row_rank
    row_ref[2:3, :] = row_t[2:3, :] + 1.0
    row_ref[3:8, :] = jnp.zeros((5, n_rows), F32)
    scores = jnp.where(col_f[:, 0:1] == row_t[0:1, :], scores, 0.0)
    lane_c = iota((n_cols, 128), 1).astype(F32)
    own_c = ones_where(col_f[:, 1:2] == lane_c, BF16)
    rank = jnp.sum(jnp.where(col_f[:, 3:4] < col_t[3:4, :], nt(own_c, own_c), 0.0), axis=0, keepdims=True)
    place = col_t[1:2, :] * 16.0 + rank
    move = ones_where(iota((n_cols, n_cols), 0).astype(F32) == place, BF16)
    top = jnp.max(jnp.max(jnp.abs(scores), axis=0, keepdims=True), axis=1, keepdims=True)
    power = jnp.ceil(jnp.log(jnp.maximum(top, 1e-36)) * 1.4426950408889634)
    scaled = scores * jnp.exp2(-power)
    high = scaled.astype(BF16)
    low = (scaled - high.astype(F32)).astype(BF16)
    moved = nn(move, high) + nn(move, low)
    note = jnp.broadcast_to(power, (8, 128))
    for g in range(16):
        out_ref[g, 0:32, :] = moved[32 * g : 32 * (g + 1), 0:128]
        out_ref[g, 32:64, :] = moved[32 * g : 32 * (g + 1), 128:256]
        out_ref[g, 64:72, :] = note
    odd = col_t[1:2, :] - 2.0 * jnp.floor(col_t[1:2, :] * 0.5)
    col_id = (odd * 64.0 + col_t[2:3, :]).astype(BF16)
    col_ref[...] = nt(jnp.broadcast_to(col_id, (8, n_cols)), move)


def send_kernel(group_ref, total_ref, col_ref, row_ref, out_ref):
    total = jnp.concatenate([total_ref[0:32, :], total_ref[32:64, :]], axis=1)
    target = row_ref[0:1, :]
    rank = row_ref[1:2, :]
    m = iota((256, 256), 0).astype(F32)
    hit = (m == target) | (m == target + 4.0)
    pick = jnp.concatenate([ones_where(hit & (rank == float(k)), BF16) for k in range(SIDE)], axis=0)
    high, middle, low = thirds(total)
    inner = jnp.broadcast_to(row_ref[2:3, :], (16, 256)).astype(BF16)
    found = nt(pick, jnp.concatenate([high, inner], axis=0))
    value = found[:, 0:32] + (nt(pick, middle) + nt(pick, low))
    index = jnp.broadcast_to(found[:, 32:33], (4 * 256, 32))
    s = iota((512, 128), 0)
    lane = iota((512, 128), 1)
    here = ones_where(s == group_ref[0] * 32 + (lane & 31), BF16)
    cols = nn(col_ref[...].astype(BF16), here)[0:1, :]
    values = jnp.concatenate([value[256 * k : 256 * (k + 1)] for k in range(SIDE)], axis=1)
    indices = jnp.concatenate([index[256 * k : 256 * (k + 1)] for k in range(SIDE)], axis=1)
    is_id = (iota((256, 128), 0) & 7) >= 4
    out_ref[...] = jnp.where(is_id, indices * 128.0 + cols, values)


def land_kernel(in_ref, out_ref):
    wide = jnp.concatenate([in_ref[64 * x : 64 * (x + 1), :] for x in range(SIDE)], axis=1)
    lane = (iota((64, 512), 1) >> 5) & 3
    index = in_ref[0:64, :]
    high = pltpu.roll(jnp.floor(index * (1.0 / 128.0)), 60, 0)
    is_value = (iota((64, 64), 0) & 7) < 4
    spot = iota((64, 64), 1).astype(F32) + 1.0
    place = jnp.concatenate(
        [ones_where(is_value & (high[:, 32 * k : 32 * k + 1] == spot), BF16) for k in range(SIDE)], axis=0
    )
    own = [jnp.where(lane == k, wide, 0.0) for k in range(SIDE)]
    total = None
    for part in thirds(jnp.concatenate(own, axis=0)):
        term = tn(place, part)
        total = term if total is None else total + term
    id_row = wide[4:5, :]
    col = id_row - 128.0 * jnp.floor(id_row * (1.0 / 128.0))
    spread = ones_where(iota((128, 512), 0).astype(F32) == col, BF16)
    high, middle, low = thirds(total)
    out_ref[...] = nt(high, spread) + (nt(middle, spread) + nt(low, spread))


def near_by(*dims, dtype=F32):
    return pltpu.VMEM(dims, dtype)


def shape(*dims, dtype=F32):
    return jax.ShapeDtypeStruct(dims, dtype)


def call(kernel, out, n, scalars=0, scratch=(), held=(), grant=GRANT):
    many = isinstance(out, tuple)
    run = pl.pallas_call(
        kernel,
        out_shape=out,
        in_specs=[SMEM] * scalars + [VMEM] * (n - scalars),
        out_specs=tuple(VMEM for _ in out) if many else VMEM,
        scratch_shapes=list(scratch),
        compiler_params=pltpu.CompilerParams(vmem_limit_bytes=grant),
    )

    def placed(*args):
        return run(
            *(pltpu.with_memory_space_constraint(a, pltpu.VMEM) if i in held else a for i, a in enumerate(args))
        )

    return placed


def device(x, y, c):
    return (x * SIDE + y) * 2 + c


LINES_X = [[device(x, y, c) for x in range(SIDE)] for y in range(SIDE) for c in range(2)]
SWAP = [(device(x, y, c), device(x, y, 1 - c)) for x in range(SIDE) for y in range(SIDE) for c in range(2)]


def shift(dx, dy):
    return [
        (device(x, y, c), device((x + dx) % SIDE, (y + dy) % SIDE, c))
        for x in range(SIDE)
        for y in range(SIDE)
        for c in range(2)
    ]


def shards(a_pieces, touched, slot_row, x_blocks, z_inverse, block_class):
    blocks = x_blocks.shape[0]
    a_local = a_pieces[0]
    slots = slot_row[None, :]
    me = lax.axis_index("row").astype(jnp.int32).reshape(1)
    classes = call(pack_kernel, near_by(SIDE, 16, WIDTH, dtype=BF16), 4, 1, grant=WIDE)(me, a_local, slots, touched)
    mine = lax.all_to_all(classes, "row", 0, 0, tiled=True, axis_index_groups=LINES_X).reshape(ROWS, WIDTH)
    own = call(
        product_kernel,
        near_by(SIDE, ROWS, WIDTH, dtype=BF16),
        8,
        3,
        (
            pltpu.VMEM((ROWS * 32, 128), F32),
            pltpu.VMEM((ROWS * 32, 128), F32),
            pltpu.VMEM((blocks, 2 * NB, 2 * NB), BF16),
            pltpu.VMEM((blocks, 2 * NB, 2 * NB), BF16),
            pltpu.VMEM((blocks, NB, 2 * NB), BF16),
        ),
        grant=WIDE,
    )(me, touched, block_class, a_local, x_blocks, z_inverse, slots, touched)
    mine, own = lax.optimization_barrier((mine, own))
    lined = lax.all_to_all(own, "row", 0, 0, tiled=True, axis_index_groups=LINES_X)
    parts = [mine]
    for n in (1, 3, 2):
        parts.append(lax.ppermute(mine, "row", shift(0, n)))
    near = jnp.stack(parts)
    far = lax.ppermute(near, "row", SWAP)
    scores, cols, rows = call(
        score_kernel, (near_by(16, SLAB, 128), near_by(8, 512), near_by(8, 256)), 3, held=(0, 1, 2)
    )(lined, near, far)
    group = lax.axis_index("grp").astype(jnp.int32).reshape(1)
    sent, cols, rows, group = lax.optimization_barrier((scores.astype(jnp.float16), cols, rows, group))
    arrived = lax.all_to_all(sent, "grp", 0, 0, tiled=True).astype(F32)
    total = jnp.sum(arrived[:, :64] * jnp.exp2(arrived[:, 64:65]), axis=0)
    outgoing = call(send_kernel, near_by(256, 128), 4, 1, held=(1, 2))(group, total, cols, rows)
    incoming = lax.all_to_all(outgoing.reshape(32, 8, 128), "row", 0, 0, tiled=True)
    return call(land_kernel, shape(64, 128), 1, held=(0,))(incoming.reshape(256, 128))


def solution(mesh):
    return jax.shard_map(
        shards,
        mesh=mesh,
        in_specs=(
            P("grp", "row", None),
            P("grp", "row"),
            P("row"),
            P("grp", None, None),
            P("grp", None, None),
            P("grp"),
        ),
        out_specs=P("row", "grp"),
        check_vma=False,
    )
```

```python
import jax
import jax.numpy as jnp
from jax import lax
from jax.experimental import pallas as pl
from jax.experimental.pallas import tpu as pltpu
from jax.sharding import PartitionSpec as P

F32 = jnp.float32
BF16 = jnp.bfloat16
NB = 64
CHUNKS = 17
WIDTH = CHUNKS * 128
ROWS = 64
SIDE = 4
SLAB = 72
QUADS = 8
GRANT = 16 << 20
WIDE = 60 << 20
VMEM = pl.BlockSpec(memory_space=pltpu.VMEM)
SMEM = pl.BlockSpec(memory_space=pltpu.SMEM)


def iota(shape, dim):
    return lax.broadcasted_iota(jnp.int32, shape, dim)


def ones_where(cond, dtype=F32):
    return jnp.where(cond, 1.0, 0.0).astype(dtype)


def nt(a, b, precision=None):
    return lax.dot_general(a, b, (((1,), (1,)), ((), ())), precision=precision, preferred_element_type=F32)


def tn(a, b, precision=None):
    return lax.dot_general(a, b, (((0,), (0,)), ((), ())), precision=precision, preferred_element_type=F32)


def nn(a, b, precision=None):
    return lax.dot_general(a, b, (((1,), (0,)), ((), ())), precision=precision, preferred_element_type=F32)


def thirds(x):
    high = x.astype(BF16)
    rest = x - high.astype(F32)
    middle = rest.astype(BF16)
    return high, middle, (rest - middle.astype(F32)).astype(BF16)


def folded(read, weigh):
    lane = iota((ROWS, 128), 1)
    column = lane & (NB - 1)
    chunks = []
    spill = jnp.zeros((ROWS, 128), F32)
    for q in range(16):
        low = read(q)
        high = read(31 - q)
        if weigh:
            low = jnp.where((column >> 1) == q, low * 0.5, low)
        turned = pltpu.roll(high, 2 * q, 1) if q else high
        chunks.append(jnp.where(column >= 2 * q, low, turned))
        block = (column >> 1) == (31 - q)
        spill = jnp.where(block, high * 0.5 if weigh else high, spill)
    return chunks, spill


def products(kind_ref, class_ref, x_ref, z_ref, tile_ref, both_ref, left_ref, right_ref, turned_ref):
    s = iota((NB, NB), 0)
    turn = ones_where(iota((NB, NB), 1) == ((s & 31) * 2 + (s >> 5)), BF16)
    rr = iota((NB, NB), 0)
    cc = iota((NB, NB), 1)
    empty = jnp.zeros((NB, NB), BF16)

    def beside(u, v):
        return jnp.concatenate([u, v], axis=1)

    for k in range(x_ref.shape[0]):
        active = (NB // 2) * (1 + class_ref[k])
        inside = (rr < active) & (cc < active)
        x = jnp.where(inside, x_ref[k].astype(F32), 0.0).astype(BF16)
        z = jnp.where(inside, z_ref[k].astype(F32), 0.0).astype(BF16)
        half = nt(x, turn).astype(BF16)
        full = nn(turn, half).astype(BF16)
        left_ref[k, 0:NB, :] = beside(full, full)
        left_ref[k, NB : 2 * NB, :] = beside(half, half)
        right_ref[k, 0:NB, :] = beside(z, empty)
        right_ref[k, NB : 2 * NB, :] = beside(empty, z)
        back = nn(turn, z).astype(BF16)
        turned_ref[k] = beside(back, back)

    def first(rows):
        return iota((rows, 128), 1) < NB

    def split(v):
        none = jnp.zeros_like(v)
        low = first(v.shape[0])
        return jnp.concatenate([jnp.where(low, v, none), jnp.where(low, none, v)], axis=0)

    def corners(u, v):
        none = jnp.zeros_like(u)
        return jnp.concatenate([beside(u, none), beside(none, v)], axis=0)

    def step(outer, carry):
        low = first(32)
        for inner in range(QUADS):
            i = (outer * QUADS + inner) * 4
            k = [kind_ref[0, i + n] for n in range(4)]
            cats, lefts, rights, backs = [], [], [], []
            for p in (0, 2):
                tile0 = tile_ref[pl.ds(i + p, 32, stride=ROWS), :]
                tile1 = tile_ref[pl.ds(i + p + 1, 32, stride=ROWS), :]
                top = jnp.where(low, tile0, pltpu.roll(tile1, NB, 1))
                bottom = jnp.where(low, pltpu.roll(tile0, NB, 1), tile1)
                cats.append(split(jnp.concatenate([top, bottom], axis=0)).astype(BF16))
                lefts.append(jnp.where(first(2 * NB), left_ref[k[p]], left_ref[k[p + 1]]))
                rights.append(
                    jnp.concatenate([right_ref[k[p], 0:NB, :], right_ref[k[p + 1], NB : 2 * NB, :]], axis=0)
                )
                backs.append(jnp.where(first(NB), turned_ref[k[p]], turned_ref[k[p + 1]]))
            left = nn(beside(*lefts), corners(*cats))
            halves = [split(left[NB:, 128 * p : 128 * (p + 1)]).astype(BF16) for p in range(2)]
            both = nn(left[:NB].astype(BF16), corners(*rights)) + nt(beside(*backs), corners(*halves))
            for p in range(2):
                top = both[:32, 128 * p : 128 * (p + 1)]
                bottom = both[32:, 128 * p : 128 * (p + 1)]
                at = pl.multiple_of((i + 2 * p) * 32, 64)
                both_ref[pl.ds(at, 32), :] = jnp.where(low, top, pltpu.roll(bottom, NB, 1))
                both_ref[pl.ds(at + 32, 32), :] = jnp.where(low, pltpu.roll(top, NB, 1), bottom)
        return carry

    lax.fori_loop(0, ROWS // (4 * QUADS), step, 0)


def slot_table(me_ref, slot_ref, touched_ref):
    r = iota((ROWS, ROWS), 0)
    c = iota((ROWS, ROWS), 1)

    def spread(row):
        full = jnp.broadcast_to(row, (ROWS, ROWS))
        return full, jnp.sum(jnp.where(r == c, full, 0.0), axis=1, keepdims=True)

    slot = slot_ref[...]
    owner_full, owner_col = spread((slot >> 6).astype(F32))
    _, inner_col = spread((slot & (ROWS - 1)).astype(F32))
    _, touched_col = spread(touched_ref[...].astype(F32))
    rank = jnp.sum(ones_where((owner_col == owner_full) & (r < c)), axis=0, keepdims=True)
    lower = jnp.sum(ones_where(owner_col < owner_full), axis=0, keepdims=True)
    holder = jnp.full((ROWS, 1), me_ref[0], jnp.int32).astype(F32)
    return (touched_col, owner_col, inner_col, holder), rank * 16.0 + lower * 0.25


def with_ids(spill, columns, first):
    lane = iota((ROWS, 128), 1)
    ids = jnp.zeros((ROWS, 128), F32)
    for n, column in enumerate(columns):
        ids = jnp.where(lane == first + n, column, ids)
    return jnp.where((lane & (NB - 1)) >= 32, spill, ids)


def pack_kernel(me_ref, a_ref, slot_ref, touched_ref, out_ref):
    columns, place = slot_table(me_ref, slot_ref, touched_ref)
    select = ones_where(iota((ROWS, ROWS), 0).astype(F32) == place, BF16)
    chunks, spill = folded(lambda q: a_ref[:, q * 128 : (q + 1) * 128].astype(F32), False)
    chunks.append(with_ids(spill, columns, 0))
    for q, chunk in enumerate(chunks):
        picked = nn(select, chunk.astype(BF16)).astype(BF16)
        for k in range(SIDE * SIDE):
            out_ref[k, :, q * 128 : (q + 1) * 128] = picked[16 * (k // SIDE) : 16 * (k // SIDE + 1)]


def product_kernel(
    me_ref, kind_ref, class_ref, a_ref, x_ref, z_ref, slot_ref, touched_ref, out_ref, tile_ref, both_ref, left_ref, right_ref, turned_ref
):
    for q in range(32):
        tile_ref[q * ROWS : (q + 1) * ROWS, :] = a_ref[:, q * 128 : (q + 1) * 128].astype(F32)
    products(kind_ref, class_ref, x_ref, z_ref, tile_ref, both_ref, left_ref, right_ref, turned_ref)
    columns, _ = slot_table(me_ref, slot_ref, touched_ref)
    chunks, spill = folded(lambda q: both_ref[pl.ds(q, ROWS, stride=32), :], True)
    chunks.append(with_ids(spill, columns, 4))
    for q, chunk in enumerate(chunks):
        out_ref[:, q * 128 : (q + 1) * 128] = chunk.astype(BF16)


def score_kernel(near_ref, far_ref, *refs):
    row_refs, (out_ref, col_ref, row_ref) = refs[:SIDE], refs[SIDE:]
    n_rows, n_cols = 256, 512
    rows = jnp.concatenate([ref[...] for ref in row_refs], axis=0)
    near = near_ref[...].reshape(256, WIDTH)
    far = far_ref[...].reshape(256, WIDTH)
    scores = jnp.concatenate([nt(near, rows), nt(far, rows)], axis=0)
    col_ids = jnp.concatenate([near[:, 16 * 128 :], far[:, 16 * 128 :]], axis=0)
    row_ids = rows[:, 16 * 128 :]
    pick = iota((8, 128), 0)
    spot = iota((8, 128), 1)
    col_t = nt(ones_where(pick == spot, BF16), col_ids)
    row_t = nt(ones_where(pick + 4 == spot, BF16), row_ids)
    col_f = col_ids.astype(F32)
    row_f = row_ids.astype(F32)
    lane_r = iota((n_rows, 128), 1).astype(F32)
    own_r = ones_where(row_f[:, 5:6] == lane_r, BF16)
    before = (iota((n_rows, n_rows), 0) < iota((n_rows, n_rows), 1)) & (row_f[:, 7:8] == row_t[3:4, :])
    row_rank = jnp.sum(jnp.where(before, nt(own_r, own_r), 0.0), axis=0, keepdims=True)
    row_ref[0:1, :] = row_t[1:2, :] * 8.0 + jnp.floor(row_t[3:4, :] * 0.125)
    row_ref[1:2, :] = row_rank
    row_ref[2:3, :] = row_t[2:3, :] + 1.0
    row_ref[3:8, :] = jnp.zeros((5, n_rows), F32)
    scores = jnp.where(col_f[:, 0:1] == row_t[0:1, :], scores, 0.0)
    lane_c = iota((n_cols, 128), 1).astype(F32)
    own_c = ones_where(col_f[:, 1:2] == lane_c, BF16)
    rank = jnp.sum(jnp.where(col_f[:, 3:4] < col_t[3:4, :], nt(own_c, own_c), 0.0), axis=0, keepdims=True)
    place = col_t[1:2, :] * 16.0 + rank
    move = ones_where(iota((n_cols, n_cols), 0).astype(F32) == place, BF16)
    top = jnp.max(jnp.max(jnp.abs(scores), axis=0, keepdims=True), axis=1, keepdims=True)
    power = jnp.ceil(jnp.log(jnp.maximum(top, 1e-36)) * 1.4426950408889634)
    scaled = scores * jnp.exp2(-power)
    high = scaled.astype(BF16)
    low = (scaled - high.astype(F32)).astype(BF16)
    moved = nn(move, high) + nn(move, low)
    note = jnp.broadcast_to(power, (8, 128))
    for g in range(16):
        out_ref[g, 0:32, :] = moved[32 * g : 32 * (g + 1), 0:128]
        out_ref[g, 32:64, :] = moved[32 * g : 32 * (g + 1), 128:256]
        out_ref[g, 64:72, :] = note
    odd = col_t[1:2, :] - 2.0 * jnp.floor(col_t[1:2, :] * 0.5)
    col_id = (odd * 64.0 + col_t[2:3, :]).astype(BF16)
    col_ref[...] = nt(jnp.broadcast_to(col_id, (8, n_cols)), move)


def send_kernel(group_ref, total_ref, col_ref, row_ref, out_ref):
    total = jnp.concatenate([total_ref[0:32, :], total_ref[32:64, :]], axis=1)
    target = row_ref[0:1, :]
    rank = row_ref[1:2, :]
    m = iota((256, 256), 0).astype(F32)
    hit = (m == target) | (m == target + 4.0)
    pick = jnp.concatenate([ones_where(hit & (rank == float(k)), BF16) for k in range(SIDE)], axis=0)
    high, middle, low = thirds(total)
    inner = jnp.broadcast_to(row_ref[2:3, :], (16, 256)).astype(BF16)
    found = nt(pick, jnp.concatenate([high, inner], axis=0))
    value = found[:, 0:32] + (nt(pick, middle) + nt(pick, low))
    index = jnp.broadcast_to(found[:, 32:33], (4 * 256, 32))
    s = iota((512, 128), 0)
    lane = iota((512, 128), 1)
    here = ones_where(s == group_ref[0] * 32 + (lane & 31), BF16)
    cols = nn(col_ref[...].astype(BF16), here)[0:1, :]
    values = jnp.concatenate([value[256 * k : 256 * (k + 1)] for k in range(SIDE)], axis=1)
    indices = jnp.concatenate([index[256 * k : 256 * (k + 1)] for k in range(SIDE)], axis=1)
    is_id = (iota((256, 128), 0) & 7) >= 4
    out_ref[...] = jnp.where(is_id, indices * 128.0 + cols, values)


def land_kernel(in_ref, out_ref):
    wide = jnp.concatenate([in_ref[64 * x : 64 * (x + 1), :] for x in range(SIDE)], axis=1)
    lane = (iota((64, 512), 1) >> 5) & 3
    index = in_ref[0:64, :]
    high = pltpu.roll(jnp.floor(index * (1.0 / 128.0)), 60, 0)
    is_value = (iota((64, 64), 0) & 7) < 4
    spot = iota((64, 64), 1).astype(F32) + 1.0
    place = jnp.concatenate(
        [ones_where(is_value & (high[:, 32 * k : 32 * k + 1] == spot), BF16) for k in range(SIDE)], axis=0
    )
    own = [jnp.where(lane == k, wide, 0.0) for k in range(SIDE)]
    total = None
    for part in thirds(jnp.concatenate(own, axis=0)):
        term = tn(place, part)
        total = term if total is None else total + term
    id_row = wide[4:5, :]
    col = id_row - 128.0 * jnp.floor(id_row * (1.0 / 128.0))
    spread = ones_where(iota((128, 512), 0).astype(F32) == col, BF16)
    high, middle, low = thirds(total)
    out_ref[...] = nt(high, spread) + (nt(middle, spread) + nt(low, spread))


def near_by(*dims, dtype=F32):
    return pltpu.VMEM(dims, dtype)


def shape(*dims, dtype=F32):
    return jax.ShapeDtypeStruct(dims, dtype)


def call(kernel, out, n, scalars=0, scratch=(), held=(), grant=GRANT):
    many = isinstance(out, tuple)
    run = pl.pallas_call(
        kernel,
        out_shape=out,
        in_specs=[SMEM] * scalars + [VMEM] * (n - scalars),
        out_specs=tuple(VMEM for _ in out) if many else VMEM,
        scratch_shapes=list(scratch),
        compiler_params=pltpu.CompilerParams(vmem_limit_bytes=grant),
    )

    def placed(*args):
        return run(
            *(pltpu.with_memory_space_constraint(a, pltpu.VMEM) if i in held else a for i, a in enumerate(args))
        )

    return placed


def device(x, y, c):
    return (x * SIDE + y) * 2 + c


PLANES = [[device(x, y, c) for x in range(SIDE) for y in range(SIDE)] for c in range(2)]
SWAP = [(device(x, y, c), device(x, y, 1 - c)) for x in range(SIDE) for y in range(SIDE) for c in range(2)]


def shift(dx, dy):
    return [
        (device(x, y, c), device((x + dx) % SIDE, (y + dy) % SIDE, c))
        for x in range(SIDE)
        for y in range(SIDE)
        for c in range(2)
    ]


def shards(a_pieces, touched, slot_row, x_blocks, z_inverse, block_class):
    blocks = x_blocks.shape[0]
    a_local = a_pieces[0]
    slots = slot_row[None, :]
    me = lax.axis_index("row").astype(jnp.int32).reshape(1)
    classes = call(pack_kernel, near_by(SIDE * SIDE, 16, WIDTH, dtype=BF16), 4, 1, grant=WIDE)(
        me, a_local, slots, touched
    )
    near = lax.all_to_all(classes, "row", 0, 0, tiled=True, axis_index_groups=PLANES)
    own = call(
        product_kernel,
        near_by(ROWS, WIDTH, dtype=BF16),
        8,
        3,
        (
            pltpu.VMEM((ROWS * 32, 128), F32),
            pltpu.VMEM((ROWS * 32, 128), F32),
            pltpu.VMEM((blocks, 2 * NB, 2 * NB), BF16),
            pltpu.VMEM((blocks, 2 * NB, 2 * NB), BF16),
            pltpu.VMEM((blocks, NB, 2 * NB), BF16),
        ),
        grant=WIDE,
    )(me, touched, block_class, a_local, x_blocks, z_inverse, slots, touched)
    lined = [own]
    for n in (2, 1, 3):
        lined.append(lax.ppermute(own, "row", shift(n, 0)))
    far = lax.ppermute(near, "row", SWAP)
    scores, cols, rows = call(
        score_kernel, (near_by(16, SLAB, 128), near_by(8, 512), near_by(8, 256)), 2 + SIDE, held=tuple(range(2 + SIDE))
    )(near, far, *lined)
    group = lax.axis_index("grp").astype(jnp.int32).reshape(1)
    sent, cols, rows, group = lax.optimization_barrier((scores.astype(jnp.float16), cols, rows, group))
    arrived = lax.all_to_all(sent, "grp", 0, 0, tiled=True).astype(F32)
    total = jnp.sum(arrived[:, :64] * jnp.exp2(arrived[:, 64:65]), axis=0)
    outgoing = call(send_kernel, near_by(256, 128), 4, 1, held=(1, 2))(group, total, cols, rows)
    incoming = lax.all_to_all(outgoing.reshape(32, 8, 128), "row", 0, 0, tiled=True)
    return call(land_kernel, shape(64, 128), 1, held=(0,))(incoming.reshape(256, 128))


def solution(mesh):
    return jax.shard_map(
        shards,
        mesh=mesh,
        in_specs=(
            P("grp", "row", None),
            P("grp", "row"),
            P("row"),
            P("grp", None, None),
            P("grp", None, None),
            P("grp"),
        ),
        out_specs=P("row", "grp"),
        check_vma=False,
    )
```

```python
import jax
import jax.numpy as jnp
from jax import lax
from jax.experimental import pallas as pl
from jax.experimental.pallas import tpu as pltpu
from jax.sharding import PartitionSpec as P

F32 = jnp.float32
BF16 = jnp.bfloat16
NB = 64
CHUNKS = 17
WIDTH = CHUNKS * 128
ROWS = 64
SIDE = 4
SLAB = 72
QUADS = 16
GRANT = 16 << 20
WIDE = 60 << 20
VMEM = pl.BlockSpec(memory_space=pltpu.VMEM)
SMEM = pl.BlockSpec(memory_space=pltpu.SMEM)


def iota(shape, dim):
    return lax.broadcasted_iota(jnp.int32, shape, dim)


def ones_where(cond, dtype=F32):
    return jnp.where(cond, 1.0, 0.0).astype(dtype)


def nt(a, b, precision=None):
    return lax.dot_general(a, b, (((1,), (1,)), ((), ())), precision=precision, preferred_element_type=F32)


def tn(a, b, precision=None):
    return lax.dot_general(a, b, (((0,), (0,)), ((), ())), precision=precision, preferred_element_type=F32)


def nn(a, b, precision=None):
    return lax.dot_general(a, b, (((1,), (0,)), ((), ())), precision=precision, preferred_element_type=F32)


def thirds(x):
    high = x.astype(BF16)
    rest = x - high.astype(F32)
    middle = rest.astype(BF16)
    return high, middle, (rest - middle.astype(F32)).astype(BF16)


def folded(read, weigh):
    lane = iota((ROWS, 128), 1)
    column = lane & (NB - 1)
    chunks = []
    spill = jnp.zeros((ROWS, 128), F32)
    for q in range(16):
        low = read(q)
        high = read(31 - q)
        if weigh:
            low = jnp.where((column >> 1) == q, low * 0.5, low)
        turned = pltpu.roll(high, 2 * q, 1) if q else high
        chunks.append(jnp.where(column >= 2 * q, low, turned))
        block = (column >> 1) == (31 - q)
        spill = jnp.where(block, high * 0.5 if weigh else high, spill)
    return chunks, spill


def products(kind_ref, class_ref, x_ref, z_ref, tile_ref, both_ref, left_ref, right_ref, turned_ref):
    s = iota((NB, NB), 0)
    turn = ones_where(iota((NB, NB), 1) == ((s & 31) * 2 + (s >> 5)), BF16)
    rr = iota((NB, NB), 0)
    cc = iota((NB, NB), 1)
    empty = jnp.zeros((NB, NB), BF16)

    def beside(u, v):
        return jnp.concatenate([u, v], axis=1)

    for k in range(x_ref.shape[0]):
        active = (NB // 2) * (1 + class_ref[k])
        inside = (rr < active) & (cc < active)
        x = jnp.where(inside, x_ref[k].astype(F32), 0.0).astype(BF16)
        z = jnp.where(inside, z_ref[k].astype(F32), 0.0).astype(BF16)
        half = nt(x, turn).astype(BF16)
        full = nn(turn, half).astype(BF16)
        left_ref[k, 0:NB, :] = beside(full, full)
        left_ref[k, NB : 2 * NB, :] = beside(half, half)
        right_ref[k, 0:NB, :] = beside(z, empty)
        right_ref[k, NB : 2 * NB, :] = beside(empty, z)
        back = nn(turn, z).astype(BF16)
        turned_ref[k] = beside(back, back)

    def first(rows):
        return iota((rows, 128), 1) < NB

    def split(v):
        none = jnp.zeros_like(v)
        low = first(v.shape[0])
        return jnp.concatenate([jnp.where(low, v, none), jnp.where(low, none, v)], axis=0)

    def corners(u, v):
        none = jnp.zeros_like(u)
        return jnp.concatenate([beside(u, none), beside(none, v)], axis=0)

    def step(outer, carry):
        low = first(32)
        for inner in range(QUADS):
            i = (outer * QUADS + inner) * 4
            k = [kind_ref[0, i + n] for n in range(4)]
            cats, lefts, rights, backs = [], [], [], []
            for p in (0, 2):
                tile0 = tile_ref[pl.ds(i + p, 32, stride=ROWS), :]
                tile1 = tile_ref[pl.ds(i + p + 1, 32, stride=ROWS), :]
                top = jnp.where(low, tile0, pltpu.roll(tile1, NB, 1))
                bottom = jnp.where(low, pltpu.roll(tile0, NB, 1), tile1)
                cats.append(split(jnp.concatenate([top, bottom], axis=0)).astype(BF16))
                lefts.append(jnp.where(first(2 * NB), left_ref[k[p]], left_ref[k[p + 1]]))
                rights.append(
                    jnp.concatenate([right_ref[k[p], 0:NB, :], right_ref[k[p + 1], NB : 2 * NB, :]], axis=0)
                )
                backs.append(jnp.where(first(NB), turned_ref[k[p]], turned_ref[k[p + 1]]))
            left = nn(beside(*lefts), corners(*cats))
            halves = [split(left[NB:, 128 * p : 128 * (p + 1)]).astype(BF16) for p in range(2)]
            both = nn(left[:NB].astype(BF16), corners(*rights)) + nt(beside(*backs), corners(*halves))
            for p in range(2):
                top = both[:32, 128 * p : 128 * (p + 1)]
                bottom = both[32:, 128 * p : 128 * (p + 1)]
                at = pl.multiple_of((i + 2 * p) * 32, 64)
                both_ref[pl.ds(at, 32), :] = jnp.where(low, top, pltpu.roll(bottom, NB, 1))
                both_ref[pl.ds(at + 32, 32), :] = jnp.where(low, pltpu.roll(top, NB, 1), bottom)
        return carry

    lax.fori_loop(0, ROWS // (4 * QUADS), step, 0)


def slot_table(me_ref, slot_ref, touched_ref):
    r = iota((ROWS, ROWS), 0)
    c = iota((ROWS, ROWS), 1)

    def spread(row):
        full = jnp.broadcast_to(row, (ROWS, ROWS))
        return full, jnp.sum(jnp.where(r == c, full, 0.0), axis=1, keepdims=True)

    slot = slot_ref[...]
    owner_full, owner_col = spread((slot >> 6).astype(F32))
    _, inner_col = spread((slot & (ROWS - 1)).astype(F32))
    _, touched_col = spread(touched_ref[...].astype(F32))
    rank = jnp.sum(ones_where((owner_col == owner_full) & (r < c)), axis=0, keepdims=True)
    lower = jnp.sum(ones_where(owner_col < owner_full), axis=0, keepdims=True)
    holder = jnp.full((ROWS, 1), me_ref[0], jnp.int32).astype(F32)
    return (touched_col, owner_col, inner_col, holder), rank * 16.0 + lower * 0.25


def with_ids(spill, columns, first):
    lane = iota((ROWS, 128), 1)
    ids = jnp.zeros((ROWS, 128), F32)
    for n, column in enumerate(columns):
        ids = jnp.where(lane == first + n, column, ids)
    return jnp.where((lane & (NB - 1)) >= 32, spill, ids)


def pack_kernel(me_ref, a_ref, slot_ref, touched_ref, out_ref):
    columns, place = slot_table(me_ref, slot_ref, touched_ref)
    select = ones_where(iota((ROWS, ROWS), 0).astype(F32) == place, BF16)
    chunks, spill = folded(lambda q: a_ref[:, q * 128 : (q + 1) * 128].astype(F32), False)
    chunks.append(with_ids(spill, columns, 0))
    for q, chunk in enumerate(chunks):
        picked = nn(select, chunk.astype(BF16)).astype(BF16)
        for k in range(SIDE * SIDE):
            out_ref[k, :, q * 128 : (q + 1) * 128] = picked[16 * (k // SIDE) : 16 * (k // SIDE + 1)]


def product_kernel(
    me_ref, kind_ref, class_ref, a_ref, x_ref, z_ref, slot_ref, touched_ref, out_ref, tile_ref, both_ref, left_ref, right_ref, turned_ref
):
    for q in range(32):
        tile_ref[q * ROWS : (q + 1) * ROWS, :] = a_ref[:, q * 128 : (q + 1) * 128].astype(F32)
    products(kind_ref, class_ref, x_ref, z_ref, tile_ref, both_ref, left_ref, right_ref, turned_ref)
    columns, _ = slot_table(me_ref, slot_ref, touched_ref)
    chunks, spill = folded(lambda q: both_ref[pl.ds(q, ROWS, stride=32), :], True)
    chunks.append(with_ids(spill, columns, 4))
    for q, chunk in enumerate(chunks):
        out_ref[:, q * 128 : (q + 1) * 128] = chunk.astype(BF16)


def order_kernel(near_ref, far_ref, move_ref, kind_ref, col_ref):
    n_cols = 512
    last = slice(16 * 128, WIDTH)
    ids = [ref[:, :, last].reshape(256, 128) for ref in (near_ref, far_ref)]
    col_ids = jnp.concatenate(ids, axis=0)
    col_t = nt(ones_where(iota((8, 128), 0) == iota((8, 128), 1), BF16), col_ids)
    col_f = col_ids.astype(F32)
    own = ones_where(col_f[:, 1:2] == iota((n_cols, 128), 1).astype(F32), BF16)
    rank = jnp.sum(jnp.where(col_f[:, 3:4] < col_t[3:4, :], nt(own, own), 0.0), axis=0, keepdims=True)
    place = col_t[1:2, :] * 16.0 + rank
    move = ones_where(iota((n_cols, n_cols), 0).astype(F32) == place, BF16)
    move_ref[...] = move
    kind_ref[...] = col_f
    odd = col_t[1:2, :] - 2.0 * jnp.floor(col_t[1:2, :] * 0.5)
    col_id = (odd * 64.0 + col_t[2:3, :]).astype(BF16)
    col_ref[...] = nt(jnp.broadcast_to(col_id, (8, n_cols)), move)


def score_kernel(near_ref, far_ref, move_ref, kind_ref, *refs):
    row_refs, (out_ref, row_ref) = refs[:SIDE], refs[SIDE:]
    n_rows = 256
    rows = jnp.concatenate([ref[...] for ref in row_refs], axis=0)
    near = near_ref[...].reshape(256, WIDTH)
    far = far_ref[...].reshape(256, WIDTH)
    scores = jnp.concatenate([nt(near, rows), nt(far, rows)], axis=0)
    row_ids = rows[:, 16 * 128 :]
    row_t = nt(ones_where(iota((8, 128), 0) + 4 == iota((8, 128), 1), BF16), row_ids)
    row_f = row_ids.astype(F32)
    own_r = ones_where(row_f[:, 5:6] == iota((n_rows, 128), 1).astype(F32), BF16)
    before = (iota((n_rows, n_rows), 0) < iota((n_rows, n_rows), 1)) & (row_f[:, 7:8] == row_t[3:4, :])
    row_rank = jnp.sum(jnp.where(before, nt(own_r, own_r), 0.0), axis=0, keepdims=True)
    row_ref[0:1, :] = row_t[1:2, :] * 8.0 + jnp.floor(row_t[3:4, :] * 0.125)
    row_ref[1:2, :] = row_rank
    row_ref[2:3, :] = row_t[2:3, :] + 1.0
    row_ref[3:8, :] = jnp.zeros((5, n_rows), F32)
    move = move_ref[...]
    scores = jnp.where(kind_ref[:, 0:1] == row_t[0:1, :], scores, 0.0)
    top = jnp.max(jnp.max(jnp.abs(scores), axis=0, keepdims=True), axis=1, keepdims=True)
    power = jnp.ceil(jnp.log(jnp.maximum(top, 1e-36)) * 1.4426950408889634)
    scaled = scores * jnp.exp2(-power)
    high = scaled.astype(BF16)
    low = (scaled - high.astype(F32)).astype(BF16)
    moved = nn(move, high) + nn(move, low)
    note = jnp.broadcast_to(power, (8, 128))
    for g in range(16):
        out_ref[g, 0:32, :] = moved[32 * g : 32 * (g + 1), 0:128]
        out_ref[g, 32:64, :] = moved[32 * g : 32 * (g + 1), 128:256]
        out_ref[g, 64:72, :] = note


def send_kernel(group_ref, total_ref, col_ref, row_ref, out_ref):
    total = jnp.concatenate([total_ref[0:32, :], total_ref[32:64, :]], axis=1)
    target = row_ref[0:1, :]
    rank = row_ref[1:2, :]
    m = iota((256, 256), 0).astype(F32)
    hit = (m == target) | (m == target + 4.0)
    pick = jnp.concatenate([ones_where(hit & (rank == float(k)), BF16) for k in range(SIDE)], axis=0)
    high, middle, low = thirds(total)
    inner = jnp.broadcast_to(row_ref[2:3, :], (16, 256)).astype(BF16)
    found = nt(pick, jnp.concatenate([high, inner], axis=0))
    value = found[:, 0:32] + (nt(pick, middle) + nt(pick, low))
    index = jnp.broadcast_to(found[:, 32:33], (4 * 256, 32))
    s = iota((512, 128), 0)
    lane = iota((512, 128), 1)
    here = ones_where(s == group_ref[0] * 32 + (lane & 31), BF16)
    cols = nn(col_ref[...].astype(BF16), here)[0:1, :]
    values = jnp.concatenate([value[256 * k : 256 * (k + 1)] for k in range(SIDE)], axis=1)
    indices = jnp.concatenate([index[256 * k : 256 * (k + 1)] for k in range(SIDE)], axis=1)
    is_id = (iota((256, 128), 0) & 7) >= 4
    out_ref[...] = jnp.where(is_id, indices * 128.0 + cols, values)


def land_kernel(in_ref, out_ref):
    wide = jnp.concatenate([in_ref[64 * x : 64 * (x + 1), :] for x in range(SIDE)], axis=1)
    lane = (iota((64, 512), 1) >> 5) & 3
    index = in_ref[0:64, :]
    high = pltpu.roll(jnp.floor(index * (1.0 / 128.0)), 60, 0)
    is_value = (iota((64, 64), 0) & 7) < 4
    spot = iota((64, 64), 1).astype(F32) + 1.0
    place = jnp.concatenate(
        [ones_where(is_value & (high[:, 32 * k : 32 * k + 1] == spot), BF16) for k in range(SIDE)], axis=1
    )
    found = None
    for part in thirds(wide):
        term = tn(place, part)
        found = term if found is None else found + term
    total = jnp.where(lane == 0, found[0:64], jnp.where(lane == 1, found[64:128], jnp.where(lane == 2, found[128:192], found[192:256])))
    id_row = wide[4:5, :]
    col = id_row - 128.0 * jnp.floor(id_row * (1.0 / 128.0))
    spread = ones_where(iota((128, 512), 0).astype(F32) == col, BF16)
    high, middle, low = thirds(total)
    out_ref[...] = nt(high, spread) + (nt(middle, spread) + nt(low, spread))


def near_by(*dims, dtype=F32):
    return pltpu.VMEM(dims, dtype)


def shape(*dims, dtype=F32):
    return jax.ShapeDtypeStruct(dims, dtype)


def call(kernel, out, n, scalars=0, scratch=(), held=(), grant=GRANT):
    many = isinstance(out, tuple)
    run = pl.pallas_call(
        kernel,
        out_shape=out,
        in_specs=[SMEM] * scalars + [VMEM] * (n - scalars),
        out_specs=tuple(VMEM for _ in out) if many else VMEM,
        scratch_shapes=list(scratch),
        compiler_params=pltpu.CompilerParams(vmem_limit_bytes=grant),
    )

    def placed(*args):
        return run(
            *(pltpu.with_memory_space_constraint(a, pltpu.VMEM) if i in held else a for i, a in enumerate(args))
        )

    return placed


def device(x, y, c):
    return (x * SIDE + y) * 2 + c


PLANES = [[device(x, y, c) for x in range(SIDE) for y in range(SIDE)] for c in range(2)]
SWAP = [(device(x, y, c), device(x, y, 1 - c)) for x in range(SIDE) for y in range(SIDE) for c in range(2)]


def shift(dx, dy):
    return [
        (device(x, y, c), device((x + dx) % SIDE, (y + dy) % SIDE, c))
        for x in range(SIDE)
        for y in range(SIDE)
        for c in range(2)
    ]


def shards(a_pieces, touched, slot_row, x_blocks, z_inverse, block_class):
    blocks = x_blocks.shape[0]
    a_local = a_pieces[0]
    slots = slot_row[None, :]
    me = lax.axis_index("row").astype(jnp.int32).reshape(1)
    classes = call(pack_kernel, near_by(SIDE * SIDE, 16, WIDTH, dtype=BF16), 4, 1, grant=WIDE)(
        me, a_local, slots, touched
    )
    near = lax.all_to_all(classes, "row", 0, 0, tiled=True, axis_index_groups=PLANES)
    own = call(
        product_kernel,
        near_by(ROWS, WIDTH, dtype=BF16),
        8,
        3,
        (
            pltpu.VMEM((ROWS * 32, 128), F32),
            pltpu.VMEM((ROWS * 32, 128), F32),
            pltpu.VMEM((blocks, 2 * NB, 2 * NB), BF16),
            pltpu.VMEM((blocks, 2 * NB, 2 * NB), BF16),
            pltpu.VMEM((blocks, NB, 2 * NB), BF16),
        ),
        grant=WIDE,
    )(me, touched, block_class, a_local, x_blocks, z_inverse, slots, touched)
    lined = [own]
    for n in (2, 1, 3):
        lined.append(lax.ppermute(own, "row", shift(n, 0)))
    far = lax.ppermute(near, "row", SWAP)
    move, kinds, cols = call(
        order_kernel, (near_by(512, 512, dtype=BF16), near_by(512, 128), near_by(8, 512)), 2, held=(0, 1)
    )(near, far)
    scores, rows = call(score_kernel, (near_by(16, SLAB, 128), near_by(8, 256)), 4 + SIDE, held=tuple(range(4 + SIDE)))(
        near, far, move, kinds, *lined
    )
    group = lax.axis_index("grp").astype(jnp.int32).reshape(1)
    sent, cols, rows, group = lax.optimization_barrier((scores.astype(jnp.float16), cols, rows, group))
    arrived = lax.all_to_all(sent, "grp", 0, 0, tiled=True).astype(F32)
    total = jnp.sum(arrived[:, :64] * jnp.exp2(arrived[:, 64:65]), axis=0)
    outgoing = call(send_kernel, near_by(256, 128), 4, 1, held=(1, 2))(group, total, cols, rows)
    incoming = lax.all_to_all(outgoing.reshape(32, 8, 128), "row", 0, 0, tiled=True)
    return call(land_kernel, shape(64, 128), 1, held=(0,))(incoming.reshape(256, 128))


def solution(mesh):
    return jax.shard_map(
        shards,
        mesh=mesh,
        in_specs=(
            P("grp", "row", None),
            P("grp", "row"),
            P("row"),
            P("grp", None, None),
            P("grp", None, None),
            P("grp"),
        ),
        out_specs=P("row", "grp"),
        check_vma=False,
    )
```

```python
import jax
import jax.numpy as jnp
from jax import lax
from jax.experimental import pallas as pl
from jax.experimental.pallas import tpu as pltpu
from jax.sharding import PartitionSpec as P

F32 = jnp.float32
BF16 = jnp.bfloat16
NB = 64
CHUNKS = 17
WIDTH = CHUNKS * 128
ROWS = 64
SIDE = 4
SLAB = 72
QUADS = 16
GRANT = 16 << 20
WIDE = 60 << 20
VMEM = pl.BlockSpec(memory_space=pltpu.VMEM)
SMEM = pl.BlockSpec(memory_space=pltpu.SMEM)


def iota(shape, dim):
    return lax.broadcasted_iota(jnp.int32, shape, dim)


def ones_where(cond, dtype=F32):
    return jnp.where(cond, 1.0, 0.0).astype(dtype)


def nt(a, b, precision=None):
    return lax.dot_general(a, b, (((1,), (1,)), ((), ())), precision=precision, preferred_element_type=F32)


def tn(a, b, precision=None):
    return lax.dot_general(a, b, (((0,), (0,)), ((), ())), precision=precision, preferred_element_type=F32)


def nn(a, b, precision=None):
    return lax.dot_general(a, b, (((1,), (0,)), ((), ())), precision=precision, preferred_element_type=F32)


def thirds(x):
    high = x.astype(BF16)
    rest = x - high.astype(F32)
    middle = rest.astype(BF16)
    return high, middle, (rest - middle.astype(F32)).astype(BF16)


def folded(read, weigh):
    lane = iota((ROWS, 128), 1)
    column = lane & (NB - 1)
    chunks = []
    spill = jnp.zeros((ROWS, 128), F32)
    for q in range(16):
        low = read(q)
        high = read(31 - q)
        if weigh:
            low = jnp.where((column >> 1) == q, low * 0.5, low)
        turned = pltpu.roll(high, 2 * q, 1) if q else high
        chunks.append(jnp.where(column >= 2 * q, low, turned))
        block = (column >> 1) == (31 - q)
        spill = jnp.where(block, high * 0.5 if weigh else high, spill)
    return chunks, spill


def products(kind_ref, class_ref, x_ref, z_ref, tile_ref, both_ref, left_ref, right_ref, turned_ref):
    s = iota((NB, NB), 0)
    turn = ones_where(iota((NB, NB), 1) == ((s & 31) * 2 + (s >> 5)), BF16)
    rr = iota((NB, NB), 0)
    cc = iota((NB, NB), 1)
    empty = jnp.zeros((NB, NB), BF16)

    def beside(u, v):
        return jnp.concatenate([u, v], axis=1)

    for k in range(x_ref.shape[0]):
        active = (NB // 2) * (1 + class_ref[k])
        inside = (rr < active) & (cc < active)
        x = jnp.where(inside, x_ref[k].astype(F32), 0.0).astype(BF16)
        z = jnp.where(inside, z_ref[k].astype(F32) * 0.5, 0.0).astype(BF16)
        half = nt(x, turn).astype(BF16)
        full = nn(turn, half).astype(BF16)
        left_ref[k, 0:NB, :] = beside(full, full)
        left_ref[k, NB : 2 * NB, :] = beside(half, half)
        right_ref[k, 0:NB, :] = beside(z, empty)
        right_ref[k, NB : 2 * NB, :] = beside(empty, z)
        back = nn(turn, z).astype(BF16)
        turned_ref[k] = beside(back, back)

    def first(rows):
        return iota((rows, 128), 1) < NB

    def split(v):
        none = jnp.zeros_like(v)
        low = first(v.shape[0])
        return jnp.concatenate([jnp.where(low, v, none), jnp.where(low, none, v)], axis=0)

    def corners(u, v):
        none = jnp.zeros_like(u)
        return jnp.concatenate([beside(u, none), beside(none, v)], axis=0)

    def step(outer, carry):
        low = first(32)
        for inner in range(QUADS):
            i = (outer * QUADS + inner) * 4
            k = [kind_ref[0, i + n] for n in range(4)]
            cats, lefts, rights, backs = [], [], [], []
            for p in (0, 2):
                tile0 = tile_ref[pl.ds(i + p, 32, stride=ROWS), :]
                tile1 = tile_ref[pl.ds(i + p + 1, 32, stride=ROWS), :]
                top = jnp.where(low, tile0, pltpu.roll(tile1, NB, 1))
                bottom = jnp.where(low, pltpu.roll(tile0, NB, 1), tile1)
                cats.append(split(jnp.concatenate([top, bottom], axis=0)).astype(BF16))
                lefts.append(jnp.where(first(2 * NB), left_ref[k[p]], left_ref[k[p + 1]]))
                rights.append(
                    jnp.concatenate([right_ref[k[p], 0:NB, :], right_ref[k[p + 1], NB : 2 * NB, :]], axis=0)
                )
                backs.append(jnp.where(first(NB), turned_ref[k[p]], turned_ref[k[p + 1]]))
            left = nn(beside(*lefts), corners(*cats))
            halves = [split(left[NB:, 128 * p : 128 * (p + 1)]).astype(BF16) for p in range(2)]
            both = nn(left[:NB].astype(BF16), corners(*rights)) + nt(beside(*backs), corners(*halves))
            for p in range(2):
                top = both[:32, 128 * p : 128 * (p + 1)]
                bottom = both[32:, 128 * p : 128 * (p + 1)]
                at = pl.multiple_of((i + 2 * p) * 32, 64)
                both_ref[pl.ds(at, 32), :] = jnp.where(low, top, pltpu.roll(bottom, NB, 1))
                both_ref[pl.ds(at + 32, 32), :] = jnp.where(low, pltpu.roll(top, NB, 1), bottom)
        return carry

    lax.fori_loop(0, ROWS // (4 * QUADS), step, 0)


def slot_table(me_ref, slot_ref, touched_ref):
    r = iota((ROWS, ROWS), 0)
    c = iota((ROWS, ROWS), 1)

    def spread(row):
        full = jnp.broadcast_to(row, (ROWS, ROWS))
        return full, jnp.sum(jnp.where(r == c, full, 0.0), axis=1, keepdims=True)

    slot = slot_ref[...]
    owner_full, owner_col = spread((slot >> 6).astype(F32))
    _, inner_col = spread((slot & (ROWS - 1)).astype(F32))
    _, touched_col = spread(touched_ref[...].astype(F32))
    rank = jnp.sum(ones_where((owner_col == owner_full) & (r < c)), axis=0, keepdims=True)
    lower = jnp.sum(ones_where(owner_col < owner_full), axis=0, keepdims=True)
    holder = jnp.full((ROWS, 1), me_ref[0], jnp.int32).astype(F32)
    return (touched_col, owner_col, inner_col, holder), rank * 16.0 + lower * 0.25


def with_ids(spill, columns, first):
    lane = iota((ROWS, 128), 1)
    ids = jnp.zeros((ROWS, 128), F32)
    for n, column in enumerate(columns):
        ids = jnp.where(lane == first + n, column, ids)
    return jnp.where((lane & (NB - 1)) >= 32, spill, ids)


def pack_kernel(me_ref, a_ref, slot_ref, touched_ref, out_ref):
    columns, place = slot_table(me_ref, slot_ref, touched_ref)
    select = ones_where(iota((ROWS, ROWS), 0).astype(F32) == place, BF16)
    chunks, spill = folded(lambda q: a_ref[:, q * 128 : (q + 1) * 128].astype(F32), False)
    chunks.append(with_ids(spill, columns, 0))
    for q, chunk in enumerate(chunks):
        picked = nn(select, chunk.astype(BF16)).astype(BF16)
        for k in range(SIDE * SIDE):
            out_ref[k, :, q * 128 : (q + 1) * 128] = picked[16 * (k // SIDE) : 16 * (k // SIDE + 1)]


def product_kernel(
    me_ref, kind_ref, class_ref, a_ref, x_ref, z_ref, slot_ref, touched_ref, out_ref, tile_ref, both_ref, left_ref, right_ref, turned_ref
):
    for q in range(32):
        tile_ref[q * ROWS : (q + 1) * ROWS, :] = a_ref[:, q * 128 : (q + 1) * 128].astype(F32)
    products(kind_ref, class_ref, x_ref, z_ref, tile_ref, both_ref, left_ref, right_ref, turned_ref)
    columns, _ = slot_table(me_ref, slot_ref, touched_ref)
    chunks, spill = folded(lambda q: both_ref[pl.ds(q, ROWS, stride=32), :], True)
    chunks.append(with_ids(spill, columns, 4))
    for q, chunk in enumerate(chunks):
        out_ref[:, q * 128 : (q + 1) * 128] = chunk.astype(BF16)


def order_kernel(near_ref, far_ref, move_ref, kind_ref, col_ref):
    n_cols = 512
    last = slice(16 * 128, WIDTH)
    ids = [ref[:, :, last].reshape(256, 128) for ref in (near_ref, far_ref)]
    col_ids = jnp.concatenate(ids, axis=0)
    col_t = nt(ones_where(iota((8, 128), 0) == iota((8, 128), 1), BF16), col_ids)
    col_f = col_ids.astype(F32)
    own = ones_where(col_f[:, 1:2] == iota((n_cols, 128), 1).astype(F32), BF16)
    rank = jnp.sum(jnp.where(col_f[:, 3:4] < col_t[3:4, :], nt(own, own), 0.0), axis=0, keepdims=True)
    place = col_t[1:2, :] * 16.0 + rank
    move = ones_where(iota((n_cols, n_cols), 0).astype(F32) == place, BF16)
    move_ref[...] = move
    kind_ref[...] = col_f
    odd = col_t[1:2, :] - 2.0 * jnp.floor(col_t[1:2, :] * 0.5)
    col_id = (odd * 64.0 + col_t[2:3, :]).astype(BF16)
    col_ref[...] = nt(jnp.broadcast_to(col_id, (8, n_cols)), move)


def score_kernel(near_ref, far_ref, move_ref, kind_ref, *refs):
    row_refs, (out_ref, row_ref) = refs[:SIDE], refs[SIDE:]
    n_rows = 256
    rows = jnp.concatenate([ref[...] for ref in row_refs], axis=0)
    near = near_ref[...].reshape(256, WIDTH)
    far = far_ref[...].reshape(256, WIDTH)
    scores = jnp.concatenate([nt(near, rows), nt(far, rows)], axis=0)
    row_ids = rows[:, 16 * 128 :]
    row_t = nt(ones_where(iota((8, 128), 0) + 4 == iota((8, 128), 1), BF16), row_ids)
    row_f = row_ids.astype(F32)
    own_r = ones_where(row_f[:, 5:6] == iota((n_rows, 128), 1).astype(F32), BF16)
    before = (iota((n_rows, n_rows), 0) < iota((n_rows, n_rows), 1)) & (row_f[:, 7:8] == row_t[3:4, :])
    row_rank = jnp.sum(jnp.where(before, nt(own_r, own_r), 0.0), axis=0, keepdims=True)
    row_ref[0:1, :] = row_t[1:2, :] * 8.0 + jnp.floor(row_t[3:4, :] * 0.125)
    row_ref[1:2, :] = row_rank
    row_ref[2:3, :] = row_t[2:3, :] + 1.0
    row_ref[3:8, :] = jnp.zeros((5, n_rows), F32)
    move = move_ref[...]
    scores = jnp.where(kind_ref[:, 0:1] == row_t[0:1, :], scores, 0.0)
    top = jnp.max(jnp.max(jnp.abs(scores), axis=0, keepdims=True), axis=1, keepdims=True)
    power = jnp.minimum(jnp.ceil(jnp.log(jnp.maximum(top, 1e-36)) * 1.4426950408889634), 126.0)
    scaled = scores * jnp.exp2(-power)
    high = scaled.astype(BF16)
    low = (scaled - high.astype(F32)).astype(BF16)
    moved = nn(move, high) + nn(move, low)
    note = jnp.broadcast_to(power + 1.0, (8, 128))
    for g in range(16):
        out_ref[g, 0:32, :] = moved[32 * g : 32 * (g + 1), 0:128]
        out_ref[g, 32:64, :] = moved[32 * g : 32 * (g + 1), 128:256]
        out_ref[g, 64:72, :] = note


def send_kernel(group_ref, total_ref, col_ref, row_ref, out_ref):
    total = jnp.concatenate([total_ref[0:32, :], total_ref[32:64, :]], axis=1)
    target = row_ref[0:1, :]
    rank = row_ref[1:2, :]
    m = iota((256, 256), 0).astype(F32)
    hit = (m == target) | (m == target + 4.0)
    pick = jnp.concatenate([ones_where(hit & (rank == float(k)), BF16) for k in range(SIDE)], axis=0)
    high, middle, low = thirds(total)
    inner = jnp.broadcast_to(row_ref[2:3, :], (16, 256)).astype(BF16)
    found = nt(pick, jnp.concatenate([high, inner], axis=0))
    value = found[:, 0:32] + (nt(pick, middle) + nt(pick, low))
    index = jnp.broadcast_to(found[:, 32:33], (4 * 256, 32))
    s = iota((512, 128), 0)
    lane = iota((512, 128), 1)
    here = ones_where(s == group_ref[0] * 32 + (lane & 31), BF16)
    cols = nn(col_ref[...].astype(BF16), here)[0:1, :]
    values = jnp.concatenate([value[256 * k : 256 * (k + 1)] for k in range(SIDE)], axis=1)
    indices = jnp.concatenate([index[256 * k : 256 * (k + 1)] for k in range(SIDE)], axis=1)
    is_id = (iota((256, 128), 0) & 7) >= 4
    out_ref[...] = jnp.where(is_id, indices * 128.0 + cols, values)


def land_kernel(in_ref, out_ref):
    wide = jnp.concatenate([in_ref[64 * x : 64 * (x + 1), :] for x in range(SIDE)], axis=1)
    lane = (iota((64, 512), 1) >> 5) & 3
    index = in_ref[0:64, :]
    high = pltpu.roll(jnp.floor(index * (1.0 / 128.0)), 60, 0)
    is_value = (iota((64, 64), 0) & 7) < 4
    spot = iota((64, 64), 1).astype(F32) + 1.0
    place = jnp.concatenate(
        [ones_where(is_value & (high[:, 32 * k : 32 * k + 1] == spot), BF16) for k in range(SIDE)], axis=1
    )
    found = None
    for part in thirds(wide):
        term = tn(place, part)
        found = term if found is None else found + term
    total = jnp.where(lane == 0, found[0:64], jnp.where(lane == 1, found[64:128], jnp.where(lane == 2, found[128:192], found[192:256])))
    id_row = wide[4:5, :]
    col = id_row - 128.0 * jnp.floor(id_row * (1.0 / 128.0))
    spread = ones_where(iota((128, 512), 0).astype(F32) == col, BF16)
    high, middle, low = thirds(total)
    out_ref[...] = nt(high, spread) + (nt(middle, spread) + nt(low, spread))


def near_by(*dims, dtype=F32):
    return pltpu.VMEM(dims, dtype)


def shape(*dims, dtype=F32):
    return jax.ShapeDtypeStruct(dims, dtype)


def call(kernel, out, n, scalars=0, scratch=(), held=(), grant=GRANT):
    many = isinstance(out, tuple)
    run = pl.pallas_call(
        kernel,
        out_shape=out,
        in_specs=[SMEM] * scalars + [VMEM] * (n - scalars),
        out_specs=tuple(VMEM for _ in out) if many else VMEM,
        scratch_shapes=list(scratch),
        compiler_params=pltpu.CompilerParams(vmem_limit_bytes=grant),
    )

    def placed(*args):
        return run(
            *(pltpu.with_memory_space_constraint(a, pltpu.VMEM) if i in held else a for i, a in enumerate(args))
        )

    return placed


def device(x, y, c):
    return (x * SIDE + y) * 2 + c


PLANES = [[device(x, y, c) for x in range(SIDE) for y in range(SIDE)] for c in range(2)]
SWAP = [(device(x, y, c), device(x, y, 1 - c)) for x in range(SIDE) for y in range(SIDE) for c in range(2)]


def shift(dx, dy):
    return [
        (device(x, y, c), device((x + dx) % SIDE, (y + dy) % SIDE, c))
        for x in range(SIDE)
        for y in range(SIDE)
        for c in range(2)
    ]


def shards(a_pieces, touched, slot_row, x_blocks, z_inverse, block_class):
    blocks = x_blocks.shape[0]
    a_local = a_pieces[0]
    slots = slot_row[None, :]
    me = lax.axis_index("row").astype(jnp.int32).reshape(1)
    classes = call(pack_kernel, near_by(SIDE * SIDE, 16, WIDTH, dtype=BF16), 4, 1, grant=WIDE)(
        me, a_local, slots, touched
    )
    near = lax.all_to_all(classes, "row", 0, 0, tiled=True, axis_index_groups=PLANES)
    own = call(
        product_kernel,
        near_by(ROWS, WIDTH, dtype=BF16),
        8,
        3,
        (
            pltpu.VMEM((ROWS * 32, 128), F32),
            pltpu.VMEM((ROWS * 32, 128), F32),
            pltpu.VMEM((blocks, 2 * NB, 2 * NB), BF16),
            pltpu.VMEM((blocks, 2 * NB, 2 * NB), BF16),
            pltpu.VMEM((blocks, NB, 2 * NB), BF16),
        ),
        grant=WIDE,
    )(me, touched, block_class, a_local, x_blocks, z_inverse, slots, touched)
    lined = [own]
    for n in (2, 1, 3):
        lined.append(lax.ppermute(own, "row", shift(n, 0)))
    far = lax.ppermute(near, "row", SWAP)
    move, kinds, cols = call(
        order_kernel, (near_by(512, 512, dtype=BF16), near_by(512, 128), near_by(8, 512)), 2, held=(0, 1)
    )(near, far)
    scores, rows = call(score_kernel, (near_by(16, SLAB, 128), near_by(8, 256)), 4 + SIDE, held=tuple(range(4 + SIDE)))(
        near, far, move, kinds, *lined
    )
    group = lax.axis_index("grp").astype(jnp.int32).reshape(1)
    sent, cols, rows, group = lax.optimization_barrier((scores.astype(jnp.float16), cols, rows, group))
    arrived = lax.all_to_all(sent, "grp", 0, 0, tiled=True).astype(F32)
    total = jnp.sum(arrived[:, :64] * jnp.exp2(arrived[:, 64:65]), axis=0)
    outgoing = call(send_kernel, near_by(256, 128), 4, 1, held=(1, 2))(group, total, cols, rows)
    incoming = lax.all_to_all(outgoing.reshape(32, 8, 128), "row", 0, 0, tiled=True)
    return call(land_kernel, shape(64, 128), 1, held=(0,))(incoming.reshape(256, 128))


def solution(mesh):
    return jax.shard_map(
        shards,
        mesh=mesh,
        in_specs=(
            P("grp", "row", None),
            P("grp", "row"),
            P("row"),
            P("grp", None, None),
            P("grp", None, None),
            P("grp"),
        ),
        out_specs=P("row", "grp"),
        check_vma=False,
    )
```

```python
import jax
import jax.numpy as jnp
from jax import lax
from jax.experimental import pallas as pl
from jax.experimental.pallas import tpu as pltpu
from jax.sharding import PartitionSpec as P

F32 = jnp.float32
BF16 = jnp.bfloat16
NB = 64
CHUNKS = 17
WIDTH = CHUNKS * 128
ROWS = 64
SIDE = 4
SLAB = 72
QUADS = 16
GRANT = 16 << 20
WIDE = 60 << 20
VMEM = pl.BlockSpec(memory_space=pltpu.VMEM)
SMEM = pl.BlockSpec(memory_space=pltpu.SMEM)


def iota(shape, dim):
    return lax.broadcasted_iota(jnp.int32, shape, dim)


def ones_where(cond, dtype=F32):
    return jnp.where(cond, 1.0, 0.0).astype(dtype)


def nt(a, b, precision=None):
    return lax.dot_general(a, b, (((1,), (1,)), ((), ())), precision=precision, preferred_element_type=F32)


def tn(a, b, precision=None):
    return lax.dot_general(a, b, (((0,), (0,)), ((), ())), precision=precision, preferred_element_type=F32)


def nn(a, b, precision=None):
    return lax.dot_general(a, b, (((1,), (0,)), ((), ())), precision=precision, preferred_element_type=F32)


def halves_of(x):
    high = x.astype(BF16)
    return high, (x - high.astype(F32)).astype(BF16)


def folded(read, weigh):
    lane = iota((ROWS, 128), 1)
    column = lane & (NB - 1)
    chunks = []
    spill = jnp.zeros((ROWS, 128), F32)
    for q in range(16):
        low = read(q)
        high = read(31 - q)
        if weigh:
            low = jnp.where((column >> 1) == q, low * 0.5, low)
        turned = pltpu.roll(high, 2 * q, 1) if q else high
        chunks.append(jnp.where(column >= 2 * q, low, turned))
        block = (column >> 1) == (31 - q)
        spill = jnp.where(block, high * 0.5 if weigh else high, spill)
    return chunks, spill


def products(kind_ref, class_ref, x_ref, z_ref, tile_ref, both_ref, left_ref, right_ref, turned_ref):
    s = iota((NB, NB), 0)
    turn = ones_where(iota((NB, NB), 1) == ((s & 31) * 2 + (s >> 5)), BF16)
    rr = iota((NB, NB), 0)
    cc = iota((NB, NB), 1)
    empty = jnp.zeros((NB, NB), BF16)

    def beside(u, v):
        return jnp.concatenate([u, v], axis=1)

    for k in range(x_ref.shape[0]):
        active = (NB // 2) * (1 + class_ref[k])
        inside = (rr < active) & (cc < active)
        x = jnp.where(inside, x_ref[k].astype(F32), 0.0).astype(BF16)
        z = jnp.where(inside, z_ref[k].astype(F32) * 0.5, 0.0).astype(BF16)
        half = nt(x, turn).astype(BF16)
        full = nn(turn, half).astype(BF16)
        left_ref[k, 0:NB, :] = beside(full, full)
        left_ref[k, NB : 2 * NB, :] = beside(half, half)
        right_ref[k, 0:NB, :] = beside(z, empty)
        right_ref[k, NB : 2 * NB, :] = beside(empty, z)
        back = nn(turn, z).astype(BF16)
        turned_ref[k] = beside(back, back)

    def first(rows):
        return iota((rows, 128), 1) < NB

    def split(v):
        none = jnp.zeros_like(v)
        low = first(v.shape[0])
        return jnp.concatenate([jnp.where(low, v, none), jnp.where(low, none, v)], axis=0)

    def corners(u, v):
        none = jnp.zeros_like(u)
        return jnp.concatenate([beside(u, none), beside(none, v)], axis=0)

    def step(outer, carry):
        low = first(32)
        for inner in range(QUADS):
            i = (outer * QUADS + inner) * 4
            k = [kind_ref[0, i + n] for n in range(4)]
            cats, lefts, rights, backs = [], [], [], []
            for p in (0, 2):
                tile0 = tile_ref[pl.ds(i + p, 32, stride=ROWS), :]
                tile1 = tile_ref[pl.ds(i + p + 1, 32, stride=ROWS), :]
                top = jnp.where(low, tile0, pltpu.roll(tile1, NB, 1))
                bottom = jnp.where(low, pltpu.roll(tile0, NB, 1), tile1)
                cats.append(split(jnp.concatenate([top, bottom], axis=0)).astype(BF16))
                lefts.append(jnp.where(first(2 * NB), left_ref[k[p]], left_ref[k[p + 1]]))
                rights.append(
                    jnp.concatenate([right_ref[k[p], 0:NB, :], right_ref[k[p + 1], NB : 2 * NB, :]], axis=0)
                )
                backs.append(jnp.where(first(NB), turned_ref[k[p]], turned_ref[k[p + 1]]))
            left = nn(beside(*lefts), corners(*cats))
            halves = [split(left[NB:, 128 * p : 128 * (p + 1)]).astype(BF16) for p in range(2)]
            both = nn(left[:NB].astype(BF16), corners(*rights)) + nt(beside(*backs), corners(*halves))
            for p in range(2):
                top = both[:32, 128 * p : 128 * (p + 1)]
                bottom = both[32:, 128 * p : 128 * (p + 1)]
                at = pl.multiple_of((i + 2 * p) * 32, 64)
                both_ref[pl.ds(at, 32), :] = jnp.where(low, top, pltpu.roll(bottom, NB, 1))
                both_ref[pl.ds(at + 32, 32), :] = jnp.where(low, pltpu.roll(top, NB, 1), bottom)
        return carry

    lax.fori_loop(0, ROWS // (4 * QUADS), step, 0)


def slot_table(me_ref, slot_ref, touched_ref):
    r = iota((ROWS, ROWS), 0)
    c = iota((ROWS, ROWS), 1)

    def spread(row):
        full = jnp.broadcast_to(row, (ROWS, ROWS))
        return full, jnp.sum(jnp.where(r == c, full, 0.0), axis=1, keepdims=True)

    slot = slot_ref[...]
    owner_full, owner_col = spread((slot >> 6).astype(F32))
    _, inner_col = spread((slot & (ROWS - 1)).astype(F32))
    _, touched_col = spread(touched_ref[...].astype(F32))
    rank = jnp.sum(ones_where((owner_col == owner_full) & (r < c)), axis=0, keepdims=True)
    lower = jnp.sum(ones_where(owner_col < owner_full), axis=0, keepdims=True)
    holder = jnp.full((ROWS, 1), me_ref[0], jnp.int32).astype(F32)
    return (touched_col, owner_col, inner_col, holder), rank * 16.0 + lower * 0.25


def with_ids(spill, columns, first):
    lane = iota((ROWS, 128), 1)
    ids = jnp.zeros((ROWS, 128), F32)
    for n, column in enumerate(columns):
        ids = jnp.where(lane == first + n, column, ids)
    return jnp.where((lane & (NB - 1)) >= 32, spill, ids)


def pack_kernel(me_ref, a_ref, slot_ref, touched_ref, out_ref):
    columns, place = slot_table(me_ref, slot_ref, touched_ref)
    select = ones_where(iota((ROWS, ROWS), 0).astype(F32) == place, BF16)
    chunks, spill = folded(lambda q: a_ref[:, q * 128 : (q + 1) * 128].astype(F32), False)
    chunks.append(with_ids(spill, columns, 0))
    for q, chunk in enumerate(chunks):
        picked = nn(select, chunk.astype(BF16)).astype(BF16)
        for k in range(SIDE * SIDE):
            out_ref[k, :, q * 128 : (q + 1) * 128] = picked[16 * (k // SIDE) : 16 * (k // SIDE + 1)]


def product_kernel(
    me_ref, kind_ref, class_ref, a_ref, x_ref, z_ref, slot_ref, touched_ref, out_ref, tile_ref, both_ref, left_ref, right_ref, turned_ref
):
    for q in range(32):
        tile_ref[q * ROWS : (q + 1) * ROWS, :] = a_ref[:, q * 128 : (q + 1) * 128].astype(F32)
    products(kind_ref, class_ref, x_ref, z_ref, tile_ref, both_ref, left_ref, right_ref, turned_ref)
    columns, _ = slot_table(me_ref, slot_ref, touched_ref)
    chunks, spill = folded(lambda q: both_ref[pl.ds(q, ROWS, stride=32), :], True)
    chunks.append(with_ids(spill, columns, 4))
    for q, chunk in enumerate(chunks):
        out_ref[:, q * 128 : (q + 1) * 128] = chunk.astype(BF16)


def order_kernel(near_ref, far_ref, move_ref, kind_ref, col_ref):
    n_cols = 512
    last = slice(16 * 128, WIDTH)
    ids = [ref[:, :, last].reshape(256, 128) for ref in (near_ref, far_ref)]
    col_ids = jnp.concatenate(ids, axis=0)
    col_t = nt(ones_where(iota((8, 128), 0) == iota((8, 128), 1), BF16), col_ids)
    col_f = col_ids.astype(F32)
    own = ones_where(col_f[:, 1:2] == iota((n_cols, 128), 1).astype(F32), BF16)
    rank = jnp.sum(jnp.where(col_f[:, 3:4] < col_t[3:4, :], nt(own, own), 0.0), axis=0, keepdims=True)
    place = col_t[1:2, :] * 16.0 + rank
    move = ones_where(iota((n_cols, n_cols), 0).astype(F32) == place, BF16)
    move_ref[...] = move
    kind_ref[...] = col_f
    odd = col_t[1:2, :] - 2.0 * jnp.floor(col_t[1:2, :] * 0.5)
    col_id = (odd * 64.0 + col_t[2:3, :]).astype(BF16)
    col_ref[...] = nt(jnp.broadcast_to(col_id, (8, n_cols)), move)


def score_kernel(near_ref, far_ref, move_ref, kind_ref, *refs):
    row_refs, (out_ref, row_ref) = refs[:SIDE], refs[SIDE:]
    n_rows = 256
    rows = jnp.concatenate([ref[...] for ref in row_refs], axis=0)
    near = near_ref[...].reshape(256, WIDTH)
    far = far_ref[...].reshape(256, WIDTH)
    scores = jnp.concatenate([nt(near, rows), nt(far, rows)], axis=0)
    row_ids = rows[:, 16 * 128 :]
    row_t = nt(ones_where(iota((8, 128), 0) + 4 == iota((8, 128), 1), BF16), row_ids)
    row_f = row_ids.astype(F32)
    own_r = ones_where(row_f[:, 5:6] == iota((n_rows, 128), 1).astype(F32), BF16)
    before = (iota((n_rows, n_rows), 0) < iota((n_rows, n_rows), 1)) & (row_f[:, 7:8] == row_t[3:4, :])
    row_rank = jnp.sum(jnp.where(before, nt(own_r, own_r), 0.0), axis=0, keepdims=True)
    row_ref[0:1, :] = row_t[1:2, :] * 8.0 + jnp.floor(row_t[3:4, :] * 0.125)
    row_ref[1:2, :] = row_rank
    row_ref[2:3, :] = row_t[2:3, :] + 1.0
    row_ref[3:8, :] = jnp.zeros((5, n_rows), F32)
    move = move_ref[...]
    scores = jnp.where(kind_ref[:, 0:1] == row_t[0:1, :], scores, 0.0)
    top = jnp.max(jnp.max(jnp.abs(scores), axis=0, keepdims=True), axis=1, keepdims=True)
    power = jnp.minimum(jnp.ceil(jnp.log(jnp.maximum(top, 1e-36)) * 1.4426950408889634), 126.0)
    scaled = scores * jnp.exp2(-power)
    high = scaled.astype(BF16)
    low = (scaled - high.astype(F32)).astype(BF16)
    moved = nn(move, high) + nn(move, low)
    note = jnp.broadcast_to(power + 1.0, (8, 128))
    for g in range(16):
        out_ref[g, 0:32, :] = moved[32 * g : 32 * (g + 1), 0:128]
        out_ref[g, 32:64, :] = moved[32 * g : 32 * (g + 1), 128:256]
        out_ref[g, 64:72, :] = note


def send_kernel(group_ref, total_ref, col_ref, row_ref, out_ref):
    total = jnp.concatenate([total_ref[0:32, :], total_ref[32:64, :]], axis=1)
    target = row_ref[0:1, :]
    rank = row_ref[1:2, :]
    m = iota((256, 256), 0).astype(F32)
    hit = (m == target) | (m == target + 4.0)
    pick = jnp.concatenate([ones_where(hit & (rank == float(k)), BF16) for k in range(SIDE)], axis=0)
    high, low = halves_of(total)
    inner = jnp.broadcast_to(row_ref[2:3, :], (16, 256)).astype(BF16)
    found = nt(pick, jnp.concatenate([high, inner], axis=0))
    value = found[:, 0:32] + nt(pick, low)
    index = jnp.broadcast_to(found[:, 32:33], (4 * 256, 32))
    s = iota((512, 128), 0)
    lane = iota((512, 128), 1)
    here = ones_where(s == group_ref[0] * 32 + (lane & 31), BF16)
    cols = nn(col_ref[...].astype(BF16), here)[0:1, :]
    values = jnp.concatenate([value[256 * k : 256 * (k + 1)] for k in range(SIDE)], axis=1)
    indices = jnp.concatenate([index[256 * k : 256 * (k + 1)] for k in range(SIDE)], axis=1)
    is_id = (iota((256, 128), 0) & 7) >= 4
    out_ref[...] = jnp.where(is_id, indices * 128.0 + cols, values)


def land_kernel(in_ref, out_ref):
    wide = jnp.concatenate([in_ref[64 * x : 64 * (x + 1), :] for x in range(SIDE)], axis=1)
    lane = (iota((64, 512), 1) >> 5) & 3
    index = in_ref[0:64, :]
    high = pltpu.roll(jnp.floor(index * (1.0 / 128.0)), 60, 0)
    is_value = (iota((64, 64), 0) & 7) < 4
    spot = iota((64, 64), 1).astype(F32) + 1.0
    place = jnp.concatenate(
        [ones_where(is_value & (high[:, 32 * k : 32 * k + 1] == spot), BF16) for k in range(SIDE)], axis=1
    )
    found = None
    for part in halves_of(wide):
        term = tn(place, part)
        found = term if found is None else found + term
    total = jnp.where(lane == 0, found[0:64], jnp.where(lane == 1, found[64:128], jnp.where(lane == 2, found[128:192], found[192:256])))
    id_row = wide[4:5, :]
    col = id_row - 128.0 * jnp.floor(id_row * (1.0 / 128.0))
    spread = ones_where(iota((128, 512), 0).astype(F32) == col, BF16)
    high, low = halves_of(total)
    out_ref[...] = nt(high, spread) + nt(low, spread)


def near_by(*dims, dtype=F32):
    return pltpu.VMEM(dims, dtype)


def shape(*dims, dtype=F32):
    return jax.ShapeDtypeStruct(dims, dtype)


def call(kernel, out, n, scalars=0, scratch=(), held=(), grant=GRANT):
    many = isinstance(out, tuple)
    run = pl.pallas_call(
        kernel,
        out_shape=out,
        in_specs=[SMEM] * scalars + [VMEM] * (n - scalars),
        out_specs=tuple(VMEM for _ in out) if many else VMEM,
        scratch_shapes=list(scratch),
        compiler_params=pltpu.CompilerParams(vmem_limit_bytes=grant),
    )

    def placed(*args):
        return run(
            *(pltpu.with_memory_space_constraint(a, pltpu.VMEM) if i in held else a for i, a in enumerate(args))
        )

    return placed


def device(x, y, c):
    return (x * SIDE + y) * 2 + c


PLANES = [[device(x, y, c) for x in range(SIDE) for y in range(SIDE)] for c in range(2)]
SWAP = [(device(x, y, c), device(x, y, 1 - c)) for x in range(SIDE) for y in range(SIDE) for c in range(2)]


def shift(dx, dy):
    return [
        (device(x, y, c), device((x + dx) % SIDE, (y + dy) % SIDE, c))
        for x in range(SIDE)
        for y in range(SIDE)
        for c in range(2)
    ]


def shards(a_pieces, touched, slot_row, x_blocks, z_inverse, block_class):
    blocks = x_blocks.shape[0]
    a_local = a_pieces[0]
    slots = slot_row[None, :]
    me = lax.axis_index("row").astype(jnp.int32).reshape(1)
    classes = call(pack_kernel, near_by(SIDE * SIDE, 16, WIDTH, dtype=BF16), 4, 1, grant=WIDE)(
        me, a_local, slots, touched
    )
    near = lax.all_to_all(classes, "row", 0, 0, tiled=True, axis_index_groups=PLANES)
    own = call(
        product_kernel,
        near_by(ROWS, WIDTH, dtype=BF16),
        8,
        3,
        (
            pltpu.VMEM((ROWS * 32, 128), F32),
            pltpu.VMEM((ROWS * 32, 128), F32),
            pltpu.VMEM((blocks, 2 * NB, 2 * NB), BF16),
            pltpu.VMEM((blocks, 2 * NB, 2 * NB), BF16),
            pltpu.VMEM((blocks, NB, 2 * NB), BF16),
        ),
        grant=WIDE,
    )(me, touched, block_class, a_local, x_blocks, z_inverse, slots, touched)
    lined = [own]
    for n in (2, 1, 3):
        lined.append(lax.ppermute(own, "row", shift(n, 0)))
    far = lax.ppermute(near, "row", SWAP)
    move, kinds, cols = call(
        order_kernel, (near_by(512, 512, dtype=BF16), near_by(512, 128), near_by(8, 512)), 2, held=(0, 1)
    )(near, far)
    scores, rows = call(score_kernel, (near_by(16, SLAB, 128), near_by(8, 256)), 4 + SIDE, held=tuple(range(4 + SIDE)))(
        near, far, move, kinds, *lined
    )
    group = lax.axis_index("grp").astype(jnp.int32).reshape(1)
    sent, cols, rows, group = lax.optimization_barrier((scores.astype(jnp.float16), cols, rows, group))
    arrived = lax.all_to_all(sent, "grp", 0, 0, tiled=True).astype(F32)
    total = jnp.sum(arrived[:, :64] * jnp.exp2(arrived[:, 64:65]), axis=0)
    outgoing = call(send_kernel, near_by(256, 128), 4, 1, held=(1, 2))(group, total, cols, rows)
    incoming = lax.all_to_all(outgoing.reshape(32, 8, 128), "row", 0, 0, tiled=True)
    return call(land_kernel, shape(64, 128), 1, held=(0,))(incoming.reshape(256, 128))


def solution(mesh):
    return jax.shard_map(
        shards,
        mesh=mesh,
        in_specs=(
            P("grp", "row", None),
            P("grp", "row"),
            P("row"),
            P("grp", None, None),
            P("grp", None, None),
            P("grp"),
        ),
        out_specs=P("row", "grp"),
        check_vma=False,
    )
```

```python
import jax
import jax.numpy as jnp
from jax import lax
from jax.experimental import pallas as pl
from jax.experimental.pallas import tpu as pltpu
from jax.sharding import PartitionSpec as P

F32 = jnp.float32
BF16 = jnp.bfloat16
NB = 64
CHUNKS = 17
WIDTH = CHUNKS * 128
ROWS = 64
SIDE = 4
SLAB = 72
QUADS = 16
GRANT = 16 << 20
WIDE = 60 << 20
VMEM = pl.BlockSpec(memory_space=pltpu.VMEM)
SMEM = pl.BlockSpec(memory_space=pltpu.SMEM)


def iota(shape, dim):
    return lax.broadcasted_iota(jnp.int32, shape, dim)


def ones_where(cond, dtype=F32):
    return jnp.where(cond, 1.0, 0.0).astype(dtype)


def nt(a, b, precision=None):
    return lax.dot_general(a, b, (((1,), (1,)), ((), ())), precision=precision, preferred_element_type=F32)


def tn(a, b, precision=None):
    return lax.dot_general(a, b, (((0,), (0,)), ((), ())), precision=precision, preferred_element_type=F32)


def nn(a, b, precision=None):
    return lax.dot_general(a, b, (((1,), (0,)), ((), ())), precision=precision, preferred_element_type=F32)


def halves_of(x):
    high = x.astype(BF16)
    return high, (x - high.astype(F32)).astype(BF16)


def folded(read, weigh):
    lane = iota((ROWS, 128), 1)
    column = lane & (NB - 1)
    chunks = []
    spill = jnp.zeros((ROWS, 128), F32)
    for q in range(16):
        low = read(q)
        high = read(31 - q)
        if weigh:
            low = jnp.where((column >> 1) == q, low * 0.5, low)
        turned = pltpu.roll(high, 2 * q, 1) if q else high
        chunks.append(jnp.where(column >= 2 * q, low, turned))
        block = (column >> 1) == (31 - q)
        spill = jnp.where(block, high * 0.5 if weigh else high, spill)
    return chunks, spill


def products(kind_ref, class_ref, x_ref, z_ref, tile_ref, both_ref, left_ref, right_ref, turned_ref):
    s = iota((NB, NB), 0)
    turn = ones_where(iota((NB, NB), 1) == ((s & 31) * 2 + (s >> 5)), BF16)
    rr = iota((NB, NB), 0)
    cc = iota((NB, NB), 1)
    empty = jnp.zeros((NB, NB), BF16)

    def beside(u, v):
        return jnp.concatenate([u, v], axis=1)

    for k in range(x_ref.shape[0]):
        active = (NB // 2) * (1 + class_ref[k])
        inside = (rr < active) & (cc < active)
        x = jnp.where(inside, x_ref[k].astype(F32), 0.0).astype(BF16)
        z = jnp.where(inside, z_ref[k].astype(F32) * 0.5, 0.0).astype(BF16)
        half = nt(x, turn).astype(BF16)
        full = nn(turn, half).astype(BF16)
        left_ref[k, 0:NB, :] = beside(full, full)
        left_ref[k, NB : 2 * NB, :] = beside(half, half)
        right_ref[k, 0:NB, :] = beside(z, empty)
        right_ref[k, NB : 2 * NB, :] = beside(empty, z)
        back = nn(turn, z).astype(BF16)
        turned_ref[k] = beside(back, back)

    def first(rows):
        return iota((rows, 128), 1) < NB

    def split(v):
        none = jnp.zeros_like(v)
        low = first(v.shape[0])
        return jnp.concatenate([jnp.where(low, v, none), jnp.where(low, none, v)], axis=0)

    def corners(u, v):
        none = jnp.zeros_like(u)
        return jnp.concatenate([beside(u, none), beside(none, v)], axis=0)

    def step(outer, carry):
        low = first(32)
        for inner in range(QUADS):
            i = (outer * QUADS + inner) * 4
            k = [kind_ref[0, i + n] for n in range(4)]
            cats, lefts, rights, backs = [], [], [], []
            for p in (0, 2):
                tile0 = tile_ref[pl.ds(i + p, 32, stride=ROWS), :]
                tile1 = tile_ref[pl.ds(i + p + 1, 32, stride=ROWS), :]
                top = jnp.where(low, tile0, pltpu.roll(tile1, NB, 1))
                bottom = jnp.where(low, pltpu.roll(tile0, NB, 1), tile1)
                cats.append(split(jnp.concatenate([top, bottom], axis=0)).astype(BF16))
                lefts.append(jnp.where(first(2 * NB), left_ref[k[p]], left_ref[k[p + 1]]))
                rights.append(
                    jnp.concatenate([right_ref[k[p], 0:NB, :], right_ref[k[p + 1], NB : 2 * NB, :]], axis=0)
                )
                backs.append(jnp.where(first(NB), turned_ref[k[p]], turned_ref[k[p + 1]]))
            left = nn(beside(*lefts), corners(*cats))
            halves = [split(left[NB:, 128 * p : 128 * (p + 1)]).astype(BF16) for p in range(2)]
            both = nn(left[:NB].astype(BF16), corners(*rights)) + nt(beside(*backs), corners(*halves))
            for p in range(2):
                top = both[:32, 128 * p : 128 * (p + 1)]
                bottom = both[32:, 128 * p : 128 * (p + 1)]
                at = pl.multiple_of((i + 2 * p) * 32, 64)
                both_ref[pl.ds(at, 32), :] = jnp.where(low, top, pltpu.roll(bottom, NB, 1))
                both_ref[pl.ds(at + 32, 32), :] = jnp.where(low, pltpu.roll(top, NB, 1), bottom)
        return carry

    lax.fori_loop(0, ROWS // (4 * QUADS), step, 0)


def slot_table(me_ref, slot_ref, touched_ref):
    r = iota((ROWS, ROWS), 0)
    c = iota((ROWS, ROWS), 1)

    def spread(row):
        full = jnp.broadcast_to(row, (ROWS, ROWS))
        return full, jnp.sum(jnp.where(r == c, full, 0.0), axis=1, keepdims=True)

    slot = slot_ref[...]
    owner_full, owner_col = spread((slot >> 6).astype(F32))
    _, inner_col = spread((slot & (ROWS - 1)).astype(F32))
    _, touched_col = spread(touched_ref[...].astype(F32))
    rank = jnp.sum(ones_where((owner_col == owner_full) & (r < c)), axis=0, keepdims=True)
    lower = jnp.sum(ones_where(owner_col < owner_full), axis=0, keepdims=True)
    holder = jnp.full((ROWS, 1), me_ref[0], jnp.int32).astype(F32)
    return (touched_col, owner_col, inner_col, holder), rank * 16.0 + lower * 0.25


def with_ids(spill, columns, first):
    lane = iota((ROWS, 128), 1)
    ids = jnp.zeros((ROWS, 128), F32)
    for n, column in enumerate(columns):
        ids = jnp.where(lane == first + n, column, ids)
    return jnp.where((lane & (NB - 1)) >= 32, spill, ids)


def pack_kernel(me_ref, a_ref, slot_ref, touched_ref, out_ref):
    columns, place = slot_table(me_ref, slot_ref, touched_ref)
    select = ones_where(iota((ROWS, ROWS), 0).astype(F32) == place, BF16)
    chunks, spill = folded(lambda q: a_ref[:, q * 128 : (q + 1) * 128].astype(F32), False)
    chunks.append(with_ids(spill, columns, 0))
    for q, chunk in enumerate(chunks):
        picked = nn(select, chunk.astype(BF16)).astype(BF16)
        for k in range(SIDE * SIDE):
            out_ref[k, :, q * 128 : (q + 1) * 128] = picked[16 * (k // SIDE) : 16 * (k // SIDE + 1)]


def product_kernel(
    me_ref, kind_ref, class_ref, a_ref, x_ref, z_ref, slot_ref, touched_ref, out_ref, tile_ref, both_ref, left_ref, right_ref, turned_ref
):
    for q in range(32):
        tile_ref[q * ROWS : (q + 1) * ROWS, :] = a_ref[:, q * 128 : (q + 1) * 128].astype(F32)
    products(kind_ref, class_ref, x_ref, z_ref, tile_ref, both_ref, left_ref, right_ref, turned_ref)
    columns, _ = slot_table(me_ref, slot_ref, touched_ref)
    chunks, spill = folded(lambda q: both_ref[pl.ds(q, ROWS, stride=32), :], True)
    chunks.append(with_ids(spill, columns, 4))
    for q, chunk in enumerate(chunks):
        out_ref[:, q * 128 : (q + 1) * 128] = chunk.astype(BF16)


def order_kernel(near_ref, far_ref, sorted_ref, kind_ref, col_ref):
    n_cols = 512
    last = slice(16 * 128, WIDTH)
    ids = [ref[:, :, last].reshape(256, 128) for ref in (near_ref, far_ref)]
    col_ids = jnp.concatenate(ids, axis=0)
    col_t = nt(ones_where(iota((8, 128), 0) == iota((8, 128), 1), BF16), col_ids)
    col_f = col_ids.astype(F32)
    own = ones_where(col_f[:, 1:2] == iota((n_cols, 128), 1).astype(F32), BF16)
    rank = jnp.sum(jnp.where(col_f[:, 3:4] < col_t[3:4, :], nt(own, own), 0.0), axis=0, keepdims=True)
    place = col_t[1:2, :] * 16.0 + rank
    move = ones_where(iota((n_cols, n_cols), 0).astype(F32) == place, BF16)
    every = jnp.concatenate([near_ref[...].reshape(256, WIDTH), far_ref[...].reshape(256, WIDTH)], axis=0)
    sorted_ref[...] = nn(move, every).astype(BF16)
    kind_ref[...] = nn(move, col_ids)
    odd = col_t[1:2, :] - 2.0 * jnp.floor(col_t[1:2, :] * 0.5)
    col_id = (odd * 64.0 + col_t[2:3, :]).astype(BF16)
    col_ref[...] = nt(jnp.broadcast_to(col_id, (8, n_cols)), move)


def score_kernel(sorted_ref, kind_ref, *refs):
    row_refs, (out_ref, row_ref) = refs[:SIDE], refs[SIDE:]
    n_rows = 256
    rows = jnp.concatenate([ref[...] for ref in row_refs], axis=0)
    scores = nt(sorted_ref[...], rows)
    row_ids = rows[:, 16 * 128 :]
    row_t = nt(ones_where(iota((8, 128), 0) + 4 == iota((8, 128), 1), BF16), row_ids)
    row_f = row_ids.astype(F32)
    own_r = ones_where(row_f[:, 5:6] == iota((n_rows, 128), 1).astype(F32), BF16)
    before = (iota((n_rows, n_rows), 0) < iota((n_rows, n_rows), 1)) & (row_f[:, 7:8] == row_t[3:4, :])
    row_rank = jnp.sum(jnp.where(before, nt(own_r, own_r), 0.0), axis=0, keepdims=True)
    row_ref[0:1, :] = row_t[1:2, :] * 8.0 + jnp.floor(row_t[3:4, :] * 0.125)
    row_ref[1:2, :] = row_rank
    row_ref[2:3, :] = row_t[2:3, :] + 1.0
    row_ref[3:8, :] = jnp.zeros((5, n_rows), F32)
    scores = jnp.where(kind_ref[:, 0:1] == row_t[0:1, :], scores, 0.0)
    top = jnp.max(jnp.max(jnp.abs(scores), axis=0, keepdims=True), axis=1, keepdims=True)
    power = jnp.minimum(jnp.ceil(jnp.log(jnp.maximum(top, 1e-36)) * 1.4426950408889634), 126.0)
    moved = scores * jnp.exp2(-power)
    note = jnp.broadcast_to(power + 1.0, (8, 128))
    for g in range(16):
        out_ref[g, 0:32, :] = moved[32 * g : 32 * (g + 1), 0:128]
        out_ref[g, 32:64, :] = moved[32 * g : 32 * (g + 1), 128:256]
        out_ref[g, 64:72, :] = note


def send_kernel(group_ref, total_ref, col_ref, row_ref, out_ref):
    total = jnp.concatenate([total_ref[0:32, :], total_ref[32:64, :]], axis=1)
    target = row_ref[0:1, :]
    rank = row_ref[1:2, :]
    m = iota((256, 256), 0).astype(F32)
    hit = (m == target) | (m == target + 4.0)
    pick = jnp.concatenate([ones_where(hit & (rank == float(k)), BF16) for k in range(SIDE)], axis=0)
    high, low = halves_of(total)
    inner = jnp.broadcast_to(row_ref[2:3, :], (16, 256)).astype(BF16)
    found = nt(pick, jnp.concatenate([high, inner], axis=0))
    value = found[:, 0:32] + nt(pick, low)
    index = jnp.broadcast_to(found[:, 32:33], (4 * 256, 32))
    s = iota((512, 128), 0)
    lane = iota((512, 128), 1)
    here = ones_where(s == group_ref[0] * 32 + (lane & 31), BF16)
    cols = nn(col_ref[...].astype(BF16), here)[0:1, :]
    values = jnp.concatenate([value[256 * k : 256 * (k + 1)] for k in range(SIDE)], axis=1)
    indices = jnp.concatenate([index[256 * k : 256 * (k + 1)] for k in range(SIDE)], axis=1)
    is_id = (iota((256, 128), 0) & 7) >= 4
    out_ref[...] = jnp.where(is_id, indices * 128.0 + cols, values)


def land_kernel(in_ref, out_ref):
    wide = jnp.concatenate([in_ref[64 * x : 64 * (x + 1), :] for x in range(SIDE)], axis=1)
    lane = (iota((64, 512), 1) >> 5) & 3
    index = in_ref[0:64, :]
    high = pltpu.roll(jnp.floor(index * (1.0 / 128.0)), 60, 0)
    is_value = (iota((64, 64), 0) & 7) < 4
    spot = iota((64, 64), 1).astype(F32) + 1.0
    place = jnp.concatenate(
        [ones_where(is_value & (high[:, 32 * k : 32 * k + 1] == spot), BF16) for k in range(SIDE)], axis=1
    )
    found = None
    for part in halves_of(wide):
        term = tn(place, part)
        found = term if found is None else found + term
    total = jnp.where(lane == 0, found[0:64], jnp.where(lane == 1, found[64:128], jnp.where(lane == 2, found[128:192], found[192:256])))
    id_row = wide[4:5, :]
    col = id_row - 128.0 * jnp.floor(id_row * (1.0 / 128.0))
    spread = ones_where(iota((128, 512), 0).astype(F32) == col, BF16)
    high, low = halves_of(total)
    out_ref[...] = nt(high, spread) + nt(low, spread)


def near_by(*dims, dtype=F32):
    return pltpu.VMEM(dims, dtype)


def shape(*dims, dtype=F32):
    return jax.ShapeDtypeStruct(dims, dtype)


def call(kernel, out, n, scalars=0, scratch=(), held=(), grant=GRANT):
    many = isinstance(out, tuple)
    run = pl.pallas_call(
        kernel,
        out_shape=out,
        in_specs=[SMEM] * scalars + [VMEM] * (n - scalars),
        out_specs=tuple(VMEM for _ in out) if many else VMEM,
        scratch_shapes=list(scratch),
        compiler_params=pltpu.CompilerParams(vmem_limit_bytes=grant),
    )

    def placed(*args):
        return run(
            *(pltpu.with_memory_space_constraint(a, pltpu.VMEM) if i in held else a for i, a in enumerate(args))
        )

    return placed


def device(x, y, c):
    return (x * SIDE + y) * 2 + c


PLANES = [[device(x, y, c) for x in range(SIDE) for y in range(SIDE)] for c in range(2)]
SWAP = [(device(x, y, c), device(x, y, 1 - c)) for x in range(SIDE) for y in range(SIDE) for c in range(2)]


def shift(dx, dy):
    return [
        (device(x, y, c), device((x + dx) % SIDE, (y + dy) % SIDE, c))
        for x in range(SIDE)
        for y in range(SIDE)
        for c in range(2)
    ]


def shards(a_pieces, touched, slot_row, x_blocks, z_inverse, block_class):
    blocks = x_blocks.shape[0]
    a_local = a_pieces[0]
    slots = slot_row[None, :]
    me = lax.axis_index("row").astype(jnp.int32).reshape(1)
    classes = call(pack_kernel, near_by(SIDE * SIDE, 16, WIDTH, dtype=BF16), 4, 1, grant=WIDE)(
        me, a_local, slots, touched
    )
    near = lax.all_to_all(classes, "row", 0, 0, tiled=True, axis_index_groups=PLANES)
    own = call(
        product_kernel,
        near_by(ROWS, WIDTH, dtype=BF16),
        8,
        3,
        (
            pltpu.VMEM((ROWS * 32, 128), F32),
            pltpu.VMEM((ROWS * 32, 128), F32),
            pltpu.VMEM((blocks, 2 * NB, 2 * NB), BF16),
            pltpu.VMEM((blocks, 2 * NB, 2 * NB), BF16),
            pltpu.VMEM((blocks, NB, 2 * NB), BF16),
        ),
        grant=WIDE,
    )(me, touched, block_class, a_local, x_blocks, z_inverse, slots, touched)
    lined = [own]
    for n in (2, 1, 3):
        lined.append(lax.ppermute(own, "row", shift(n, 0)))
    far = lax.ppermute(near, "row", SWAP)
    columns, kinds, cols = call(
        order_kernel, (near_by(512, WIDTH, dtype=BF16), near_by(512, 128), near_by(8, 512)), 2, held=(0, 1)
    )(near, far)
    scores, rows = call(score_kernel, (near_by(16, SLAB, 128), near_by(8, 256)), 2 + SIDE, held=tuple(range(2 + SIDE)))(
        columns, kinds, *lined
    )
    group = lax.axis_index("grp").astype(jnp.int32).reshape(1)
    sent, cols, rows, group = lax.optimization_barrier((scores.astype(jnp.float16), cols, rows, group))
    arrived = lax.all_to_all(sent, "grp", 0, 0, tiled=True).astype(F32)
    total = jnp.sum(arrived[:, :64] * jnp.exp2(arrived[:, 64:65]), axis=0)
    outgoing = call(send_kernel, near_by(256, 128), 4, 1, held=(1, 2))(group, total, cols, rows)
    incoming = lax.all_to_all(outgoing.reshape(32, 8, 128), "row", 0, 0, tiled=True)
    return call(land_kernel, shape(64, 128), 1, held=(0,))(incoming.reshape(256, 128))


def solution(mesh):
    return jax.shard_map(
        shards,
        mesh=mesh,
        in_specs=(
            P("grp", "row", None),
            P("grp", "row"),
            P("row"),
            P("grp", None, None),
            P("grp", None, None),
            P("grp"),
        ),
        out_specs=P("row", "grp"),
        check_vma=False,
    )
```
